256 devices in a mesh: tmpl: 32 (over x, y, core), grid: 8 (over z).
Axes of the slice: x: 4, y: 4, z: 8, core: 2. Of those that a mesh axis runs over, the one named last changes fastest.
Arguments:
- spectrum: float32 [1024, 64, 64, 128], P('tmpl', 'grid'), may hold values from -12 to 12
Outputs:
- best_scores: float32 [4, 64, 64, 64], P(None, 'grid', 'tmpl')
- coherence: float32 [64, 64, 64], P('grid', 'tmpl')
The draws below stay inside these ranges and needn't reach their ends.
All inputs are finite; a program needn't handle non-finite values.
Results may differ from the reference program's by a relative error of at most 0.0001.
Values sent between devices are 32-bit elements; how exact they have to be, the bound alone decides.
A program may use at most 128 MiB of HBM per device.

```python
import math
import jax
import jax.numpy as jnp
from jax import lax

NG = 64
TEMPLATES = 1024
TOP = 4


def log_uniform(key, shape, low, high):
    return jnp.exp(jax.random.uniform(key, shape, jnp.float32, math.log(low), math.log(high)))


def draw_spectrum(key, part):
    streams = jax.random.split(jax.random.fold_in(key, 11), 8)
    shape = (TEMPLATES, NG, NG, 2 * NG)
    base = jnp.clip(0.125 * jax.random.normal(streams[0], shape, jnp.float32), -0.75, 0.75)
    factor = log_uniform(streams[1], (TEMPLATES, NG, 1, 1), 0.5, 2.0)
    offset = jax.random.normal(streams[3], (TEMPLATES, NG), jnp.float32)
    values = base * factor
    values = values.at[:, :, :, 0].add(offset[:, :, None])
    return jnp.clip(values, -12.0, 12.0)


def setup_inputs(seed: int = 0) -> dict:
    streams_of = jax.random.split(jax.random.key(seed), 2)
    spectrum = draw_spectrum(jax.random.fold_in(streams_of[1], 71), 0)
    return dict(spectrum=spectrum)


FLOOR = -1e+30
SPREAD_FLOOR = 0.25

def phase_table(length):
    order = jnp.arange(length, dtype=jnp.int32)
    turns = order[:, None] * order[None, :] % length
    angle = turns.astype(jnp.float32) * (2.0 * math.pi / length)
    return jnp.concatenate([jnp.cos(angle), -jnp.sin(angle)], axis=0)

def merge_top(former, latter):
    result = []
    for rank_out in range(len(former)):
        winner = jnp.maximum(former[rank_out], latter[rank_out])
        for rank_in in range(rank_out):
            winner = jnp.maximum(winner, jnp.minimum(former[rank_in], latter[rank_out - rank_in - 1]))
        result.append(winner)
    return tuple(result)

def reference(spectrum):
    table = phase_table(NG)
    cell_count = float(NG * NG * NG)

    def advance(carry, coeffs):
        leaders, running = carry
        score = jnp.dot(coeffs.reshape(NG * NG, 2 * NG), table, precision=lax.Precision.HIGHEST, preferred_element_type=jnp.float32).reshape(NG, NG, NG)
        average = jnp.sum(score) / cell_count
        centred = score - average
        spread = jnp.sum(centred * centred) / cell_count
        normed = centred / jnp.sqrt(spread + SPREAD_FLOOR)
        filler = jnp.full((NG, NG, NG), FLOOR, jnp.float32)
        single = (normed,) + tuple((filler for rank_in in range(TOP - 1)))
        return ((merge_top(leaders, single), running + normed), None)
    start = tuple((jnp.full((NG, NG, NG), FLOOR, jnp.float32) for rank_in in range(TOP)))
    (leaders, running), unused = lax.scan(advance, (start, jnp.zeros((NG, NG, NG), jnp.float32)), spectrum)
    return (jnp.stack(leaders, axis=0), running / math.sqrt(TEMPLATES))
```

```python
import functools
import math

import jax
import jax.numpy as jnp
import numpy as np
from jax import lax
from jax.experimental import pallas as pl
from jax.experimental.pallas import tpu as pltpu
from jax.sharding import PartitionSpec as P

TOP = 4
SPREAD_FLOOR = 0.25
LANES = 128
CHUNK = 2
PARTS = TOP + 1


def phase_table(points):
    order = np.arange(points)
    angle = (order[:, None] * order[None, :] % points) * (2.0 * math.pi / points)
    table = np.concatenate([np.cos(angle), -np.sin(angle)], axis=0).astype(np.float32)
    high = table.astype(jnp.bfloat16)
    low = (table - high.astype(np.float32)).astype(jnp.bfloat16)
    pair = lambda part: np.kron(np.eye(2, dtype=np.float32), part.astype(np.float32))
    half = np.concatenate([pair(high), pair(low)], axis=1)
    return np.concatenate([half, half], axis=0).astype(jnp.bfloat16)


def swap(a, b):
    return jnp.maximum(a, b), jnp.minimum(a, b)


def sort_four(a, b, c, d):
    a, b = swap(a, b)
    c, d = swap(c, d)
    a, c = swap(a, c)
    b, d = swap(b, d)
    b, c = swap(b, c)
    return a, b, c, d


def merge_four(first, second):
    a, b, c, d = (jnp.maximum(first[i], second[3 - i]) for i in range(4))
    a, c = swap(a, c)
    b, d = swap(b, d)
    a, b = swap(a, b)
    c, d = swap(c, d)
    return a, b, c, d


def kernel(
    sizes,
    x_hbm,
    table_hbm,
    out_ref,
    x_buf,
    table,
    score,
    other,
    part_sum,
    part_sq,
    stat,
    scale,
    shift,
    mine,
    got,
    x_sem,
    table_sem,
    pair_send,
    pair_recv,
    stat_send,
    stat_recv,
    list_send,
    list_recv,
):
    nx, ny, nz, local = sizes
    chunks = local // CHUNK
    rows = 8
    lines = nx * 8
    places = (nx // 2) * rows
    piece = PARTS * rows
    count = float((2 * lines) ** 3)

    me = lax.axis_index("tmpl")
    z = lax.axis_index("grid")
    chip = me // 2
    core = lax.rem(me, 2)
    x = chip // ny
    sibling = me + 1 - 2 * core

    def load(k):
        return pltpu.make_async_copy(
            x_hbm.at[pl.ds(k * CHUNK, CHUNK)], x_buf.at[pl.ds(k * CHUNK, CHUNK)], x_sem.at[k]
        )

    load(0).start()
    table_copy = pltpu.make_async_copy(table_hbm, table, table_sem)
    table_copy.start()

    @pl.loop(1, chunks)
    def _(k):
        load(k).start()

    barrier = pltpu.get_barrier_semaphore()
    groups = 2 * nx * ny

    @pl.loop(1, groups)
    def _(k):
        pl.semaphore_signal(barrier, inc=1, device_id={"tmpl": lax.rem(me + k, groups), "grid": z})

    @pl.loop(1, nz)
    def _(k):
        for c in range(2):
            pl.semaphore_signal(
                barrier, inc=1, device_id={"tmpl": 2 * chip + c, "grid": lax.rem(z + k, nz)}
            )

    def pair_copy(k):
        part = pl.ds(k * CHUNK, CHUNK)
        return pltpu.make_async_remote_copy(
            src_ref=score.at[1 - core, part],
            dst_ref=other.at[part],
            send_sem=pair_send.at[k],
            recv_sem=pair_recv.at[k],
            device_id={"tmpl": sibling, "grid": z},
        )

    table_copy.wait()

    @pl.loop(0, chunks)
    def _(k):
        load(k).wait()
        for i in range(CHUNK):
            t = k * CHUNK + i
            operands = []
            lows = []
            for parity in range(2):
                value = x_buf[t, :, pl.ds(parity, lines, stride=2), :].reshape(rows * lines, LANES)
                high = value.astype(jnp.bfloat16)
                operands.append(high)
                lows.append((value - high.astype(jnp.float32)).astype(jnp.bfloat16))
            lhs = jnp.concatenate(operands + lows, axis=1)
            product = jnp.dot(lhs, table[...], preferred_element_type=jnp.float32)
            value = product[:, :LANES] + product[:, LANES:]
            value = value.reshape(rows, nx, 8, LANES)
            for g in range(nx):
                h, q = g // (nx // 2), g % (nx // 2)
                score[h, t, pl.ds(q * rows, rows)] = value[:, g]
            flat = value.reshape(rows * nx, 8, LANES)
            part_sum[pl.ds(t, 1)] = jnp.sum(jnp.sum(flat, axis=0), axis=0, keepdims=True)
            part_sq[pl.ds(t, 1)] = jnp.sum(jnp.sum(flat * flat, axis=0), axis=0, keepdims=True)

    pl.semaphore_wait(barrier, groups - 1 + 2 * (nz - 1))

    lane = lax.broadcasted_iota(jnp.int32, (local, LANES), 1)
    line = lax.broadcasted_iota(jnp.int32, (local, LANES), 0)
    sums = jnp.sum(part_sum[...], axis=1, keepdims=True)
    squares = jnp.sum(part_sq[...], axis=1, keepdims=True)
    spread_out = jnp.where(lane == line, sums, 0.0) + jnp.where(lane == line + 64, squares, 0.0)
    own = core * nz + z
    stat[own] = jnp.sum(spread_out, axis=0, keepdims=True)

    @pl.loop(0, chunks)
    def _(k):
        pair_copy(k).start()

    def stat_copy(slot, c, peer_z):
        return pltpu.make_async_remote_copy(
            src_ref=stat.at[slot],
            dst_ref=stat.at[slot],
            send_sem=stat_send.at[c * nz + peer_z],
            recv_sem=stat_recv.at[slot],
            device_id={"tmpl": 2 * chip + c, "grid": peer_z},
        )

    hops = sorted(range(nz), key=lambda k: -min(k, nz - k))
    for k in hops:
        peer_z = lax.rem(z + k, nz)
        for flip in range(2):
            if k or flip:
                stat_copy(own, core * (1 - flip) + (1 - core) * flip, peer_z).start()
    for k in hops:
        peer_z = lax.rem(z + k, nz)
        for flip in range(2):
            if k or flip:
                c = core * (1 - flip) + (1 - core) * flip
                stat_copy(c * nz + peer_z, c, peer_z).wait_recv()

    for side in range(2):
        c = core * (1 - side) + (1 - core) * side
        row = stat[c * nz]
        for k in range(1, nz):
            row = row + stat[c * nz + k]
        row = jnp.broadcast_to(row, (local, LANES))
        total = jnp.sum(jnp.where(lane == line, row, 0.0), axis=1, keepdims=True)
        square = jnp.sum(jnp.where(lane == line + 64, row, 0.0), axis=1, keepdims=True)
        average = total / count
        spread = square / count - average * average
        factor = 1.0 / jnp.sqrt(spread + SPREAD_FLOOR)
        scale[side] = jnp.broadcast_to(factor, (local, LANES))
        shift[side] = jnp.broadcast_to(-average * factor, (local, LANES))

    @pl.loop(0, chunks)
    def _(k):
        pair_copy(k).wait_recv()

    def list_copy(dest, slot_sem):
        return pltpu.make_async_remote_copy(
            src_ref=mine.at[pl.ds(dest * piece, piece)],
            dst_ref=got.at[pl.ds(chip * piece, piece)],
            send_sem=list_send.at[dest],
            recv_sem=list_recv.at[chip],
            device_id={"tmpl": core * (nx * ny) + dest, "grid": z},
        )

    targets = nx * ny
    block = 4

    for q in range(nx // 2):
        for first in range(0, rows, block):
            where = q * rows + first

            def step(n, carry):
                carry = list(carry)
                t = n * 2
                values = []
                for side in range(2):
                    for j in range(2):
                        a = scale[side, pl.ds(t + j, 1), :]
                        b = shift[side, pl.ds(t + j, 1), :]
                        raw = (
                            score[core, t + j, pl.ds(where, block)]
                            if side == 0
                            else other[t + j, pl.ds(where, block)]
                        )
                        values.append(raw * a + b)
                for p in range(block):
                    four = [v[p] for v in values]
                    best = merge_four(carry[p][:TOP], sort_four(*four))
                    carry[p] = best + (carry[p][TOP] + ((four[0] + four[1]) + (four[2] + four[3])),)
                return tuple(carry)

            low = jnp.full((8, LANES), -jnp.inf, jnp.float32)
            start = tuple((low,) * TOP + (jnp.zeros((8, LANES), jnp.float32),) for _ in range(block))
            result = lax.fori_loop(0, local // 2, step, start)
            for p in range(block):
                for part in range(PARTS):
                    mine[pl.ds(q * 8 * piece + part * rows + first + p, 8, stride=piece), :] = result[p][part]

        @pl.loop(0, 8)
        def _(s):
            dest = q * 8 + s

            @pl.when(core * targets + dest != me)
            def _():
                list_copy(dest, chip).start()

    source_core = x // (nx // 2)

    @pl.when(source_core == core)
    def _():
        got[pl.ds(chip * piece, piece), :] = mine[pl.ds((me - core * targets) * piece, piece), :]

    @pl.loop(0, targets)
    def _(q):
        @pl.when(2 * q + source_core != me)
        def _():
            pltpu.make_async_remote_copy(
                src_ref=mine.at[pl.ds(0, piece)],
                dst_ref=got.at[pl.ds(q * piece, piece)],
                send_sem=list_send.at[0],
                recv_sem=list_recv.at[q],
                device_id={"tmpl": 2 * q + source_core, "grid": z},
            ).wait_recv()

    lists = []
    total = None
    for q in range(targets):
        parts = [got[q * piece + rows * k : q * piece + rows * (k + 1), :] for k in range(PARTS)]
        lists.append(parts[:TOP])
        total = parts[TOP] if total is None else total + parts[TOP]
    while len(lists) > 1:
        lists = [merge_four(a, b) for a, b in zip(lists[::2], lists[1::2])]
    for k in range(TOP):
        out_ref[k] = lists[0][k]
    out_ref[TOP] = total * (1.0 / math.sqrt(2 * targets * local))

    @pl.loop(0, chunks)
    def _(k):
        pair_copy(k).wait_send()

    for k in hops:
        peer_z = lax.rem(z + k, nz)
        for flip in range(2):
            if k or flip:
                stat_copy(own, core * (1 - flip) + (1 - core) * flip, peer_z).wait_send()

    @pl.loop(0, targets)
    def _(dest):
        @pl.when(core * targets + dest != me)
        def _():
            list_copy(dest, chip).wait_send()


def body(sizes, spectrum):
    nx, ny, nz, local = sizes
    points = spectrum.shape[3] // 2
    rows = spectrum.shape[1]
    lines = spectrum.shape[2] // 2
    table = jnp.asarray(phase_table(points))
    places = (nx // 2) * rows
    piece = PARTS * rows
    targets = nx * ny
    dma = pltpu.SemaphoreType.DMA
    out = pl.pallas_call(
        functools.partial(kernel, sizes),
        out_shape=jax.ShapeDtypeStruct((PARTS, rows, LANES), jnp.float32),
        in_specs=[pl.BlockSpec(memory_space=pl.ANY)] * 2,
        out_specs=pl.BlockSpec(memory_space=pltpu.VMEM),
        scratch_shapes=[
            pltpu.VMEM(spectrum.shape, jnp.float32),
            pltpu.VMEM(table.shape, jnp.bfloat16),
            pltpu.VMEM((2, local, places, 8, LANES), jnp.float32),
            pltpu.VMEM((local, places, 8, LANES), jnp.float32),
            pltpu.VMEM((local, LANES), jnp.float32),
            pltpu.VMEM((local, LANES), jnp.float32),
            pltpu.VMEM((2 * nz, 1, LANES), jnp.float32),
            pltpu.VMEM((2, local, LANES), jnp.float32),
            pltpu.VMEM((2, local, LANES), jnp.float32),
            pltpu.VMEM((targets * piece, LANES), jnp.float32),
            pltpu.VMEM((targets * piece, LANES), jnp.float32),
            dma((local // CHUNK,)),
            dma,
            dma((local // CHUNK,)),
            dma((local // CHUNK,)),
            dma((2 * nz,)),
            dma((2 * nz,)),
            dma((targets,)),
            dma((targets,)),
        ],
        compiler_params=pltpu.CompilerParams(
            collective_id=0, has_side_effects=True, vmem_limit_bytes=40 * 1024 * 1024
        ),
    )(spectrum, table)
    out = out.reshape(PARTS, rows, 2, points)
    return out[:TOP], out[TOP]


def build(mesh, nx, ny):
    nz = mesh.shape["grid"]

    def run(spectrum):
        sizes = (nx, ny, nz, spectrum.shape[0] // mesh.shape["tmpl"])
        return jax.shard_map(
            functools.partial(body, sizes),
            mesh=mesh,
            in_specs=(P("tmpl", "grid", None, None),),
            out_specs=(P(None, "grid", "tmpl", None), P("grid", "tmpl", None)),
            check_vma=False,
        )(spectrum)

    return run


def solution(mesh):
    return build(mesh, 4, 4)
```

```python
import functools
import math

import jax
import jax.numpy as jnp
from jax import lax
from jax.experimental import pallas as pl
from jax.experimental.pallas import tpu as pltpu
from jax.sharding import PartitionSpec as P

TOP = 4
SPREAD_FLOOR = 0.25
LANES = 128
CHUNK = 2
PARTS = TOP + 1
MESH = pl.DeviceIdType.MESH


def groups_of(local):
    return (4, 8, 8, 8, 4) if local == 32 else (local // 2, local // 2)


def fill_table(table, points):
    shape = (2 * points, LANES)
    row = lax.broadcasted_iota(jnp.int32, shape, 0)
    lane = lax.broadcasted_iota(jnp.int32, shape, 1)
    quarter = jnp.where(row >= points, points // 4, 0)
    turns = ((row & (points - 1)) * (lane & (points - 1)) + quarter) & (points - 1)
    turns = jnp.where(turns > points // 2, turns - points, turns)
    value = jnp.cos(turns.astype(jnp.float32) * (2.0 * math.pi / points))
    high = value.astype(jnp.bfloat16).astype(jnp.float32)
    for parity in range(2):
        keep = (lane >= points) == bool(parity)
        rows = pl.ds(parity * 2 * points, 2 * points)
        table[rows, 0:LANES] = jnp.where(keep, high, 0.0).astype(jnp.bfloat16)
        table[rows, LANES:] = jnp.where(keep, value - high, 0.0).astype(jnp.bfloat16)


def swap(a, b):
    return jnp.maximum(a, b), jnp.minimum(a, b)


def sort_four(a, b, c, d):
    a, b = swap(a, b)
    c, d = swap(c, d)
    a, c = swap(a, c)
    b, d = swap(b, d)
    b, c = swap(b, c)
    return a, b, c, d


def merge_four(first, second):
    a, b, c, d = (jnp.maximum(first[i], second[3 - i]) for i in range(4))
    a, c = swap(a, c)
    b, d = swap(b, d)
    a, b = swap(a, b)
    c, d = swap(c, d)
    return a, b, c, d


def kernel(
    sizes,
    x_hbm,
    out_ref,
    x_buf,
    table,
    score,
    other,
    part_sum,
    part_sq,
    stat,
    scale,
    shift,
    kept,
    mine,
    got,
    x_sem,
    pair_send,
    pair_recv,
    stat_send,
    stat_recv,
    list_send,
    list_recv,
):
    nx, ny, nz, local = sizes
    chunks = local // CHUNK
    rows = 8
    lines = nx * 8
    piece = PARTS * rows
    targets = nx * ny
    count = float((2 * lines) ** 3)
    sizes_of = groups_of(local)
    groups = len(sizes_of)
    starts = [sum(sizes_of[:g]) for g in range(groups)]
    slots = 2 * nz

    me = lax.axis_index("tmpl")
    z = lax.axis_index("grid")
    chip = me // 2
    core = lax.rem(me, 2)
    x = chip // ny
    y = lax.rem(chip, ny)
    sibling = me + 1 - 2 * core
    plane = 2 * targets
    own = core * nz + z

    def load(k):
        return pltpu.make_async_copy(
            x_hbm.at[pl.ds(k * CHUNK, CHUNK)], x_buf.at[pl.ds(k * CHUNK, CHUNK)], x_sem.at[k]
        )

    @pl.loop(0, chunks)
    def _(k):
        load(k).start()

    barrier = pltpu.get_barrier_semaphore()

    @pl.loop(1, nz)
    def _(k):
        for c in range(2):
            peer = {"tmpl": 2 * chip + c, "grid": lax.rem(z + k, nz)}
            pl.semaphore_signal(barrier, inc=1, device_id=peer, device_id_type=MESH)

    @pl.loop(1, plane)
    def _(k):
        peer = {"tmpl": lax.rem(me + k, plane), "grid": z}
        pl.semaphore_signal(barrier, inc=1, device_id=peer, device_id_type=MESH)

    fill_table(table, x_hbm.shape[3] // 2)

    def pair_copy(g):
        part = pl.ds(starts[g], sizes_of[g])
        return pltpu.make_async_remote_copy(
            src_ref=score.at[1 - core, part],
            dst_ref=other.at[part],
            send_sem=pair_send.at[g],
            recv_sem=pair_recv.at[g],
            device_id={"tmpl": sibling, "grid": z},
            device_id_type=MESH,
        )

    def transform(g):
        weights = table[...]
        for t in range(starts[g], starts[g] + sizes_of[g]):
            if t % CHUNK == 0:
                load(t // CHUNK).wait()
        for t in range(starts[g], starts[g] + sizes_of[g]):
            highs = []
            lows = []
            for parity in range(2):
                value = x_buf[t, :, pl.ds(parity, lines, stride=2), :].reshape(rows * lines, LANES)
                high = value.astype(jnp.bfloat16)
                highs.append(high)
                lows.append((value - high.astype(jnp.float32)).astype(jnp.bfloat16))
            product = jnp.dot(
                jnp.concatenate(highs, axis=1), weights, preferred_element_type=jnp.float32
            ) + jnp.dot(jnp.concatenate(lows, axis=1), weights, preferred_element_type=jnp.float32)
            value = product[:, :LANES] + product[:, LANES:]
            value = value.reshape(rows, nx, 8, LANES)
            for b in range(nx):
                h, q = b // (nx // 2), b % (nx // 2)
                score[h, t, pl.ds(q * rows, rows)] = value[:, b]
            flat = value.reshape(rows * nx, 8, LANES)
            part_sum[pl.ds(t, 1)] = jnp.sum(jnp.sum(flat, axis=0), axis=0, keepdims=True)
            part_sq[pl.ds(t, 1)] = jnp.sum(jnp.sum(flat * flat, axis=0), axis=0, keepdims=True)

    def masks(n):
        lane = lax.broadcasted_iota(jnp.int32, (n, LANES), 1)
        line = lax.broadcasted_iota(jnp.int32, (n, LANES), 0)
        return lane == line, lane == line + LANES // 2

    hops = sorted(range(nz), key=lambda k: -min(k, nz - k))

    def peers():
        for k in hops:
            peer_z = lax.rem(z + k, nz)
            for flip in range(2):
                if k or flip:
                    c = core if flip == 0 else 1 - core
                    yield c, peer_z

    def stat_copy(g, slot, c, peer_z):
        return pltpu.make_async_remote_copy(
            src_ref=stat.at[g * slots + slot],
            dst_ref=stat.at[g * slots + slot],
            send_sem=stat_send.at[g * slots + c * nz + peer_z],
            recv_sem=stat_recv.at[g * slots + slot],
            device_id={"tmpl": 2 * chip + c, "grid": peer_z},
            device_id_type=MESH,
        )

    def share_stats(g):
        part = pl.ds(starts[g], sizes_of[g])
        first, second = masks(sizes_of[g])
        sums = jnp.sum(part_sum[part], axis=1, keepdims=True)
        squares = jnp.sum(part_sq[part], axis=1, keepdims=True)
        line = jnp.where(first, sums, 0.0) + jnp.where(second, squares, 0.0)
        stat[g * slots + own] = jnp.sum(line, axis=0, keepdims=True)
        for c, peer_z in peers():
            stat_copy(g, own, c, peer_z).start()

    def norms(g):
        for c, peer_z in peers():
            stat_copy(g, c * nz + peer_z, c, peer_z).wait_recv()
        part = pl.ds(starts[g], sizes_of[g])
        n = sizes_of[g]
        first, second = masks(n)
        for side in range(2):
            c = core if side == 0 else 1 - core
            line = stat[g * slots + c * nz]
            for k in range(1, nz):
                line = line + stat[g * slots + c * nz + k]
            line = jnp.broadcast_to(line, (n, LANES))
            total = jnp.sum(jnp.where(first, line, 0.0), axis=1, keepdims=True)
            square = jnp.sum(jnp.where(second, line, 0.0), axis=1, keepdims=True)
            average = total / count
            spread = square / count - average * average
            factor = 1.0 / jnp.sqrt(spread + SPREAD_FLOOR)
            scale[side, part] = jnp.broadcast_to(factor, (n, LANES))
            shift[side, part] = jnp.broadcast_to(-average * factor, (n, LANES))

    block = 4
    blocks = (nx // 2) * rows // block

    def best_of(g, where):
        carry = None
        if g:
            carry = [tuple(kept[where + p, k] for k in range(PARTS)) for p in range(block)]
        for t in range(starts[g], starts[g] + sizes_of[g], 2):
            values = []
            for side in range(2):
                for j in range(2):
                    a = scale[side, pl.ds(t + j, 1), :]
                    b = shift[side, pl.ds(t + j, 1), :]
                    at = pl.ds(where, block)
                    raw = score[core, t + j, at] if side == 0 else other[t + j, at]
                    values.append(raw * a + b)
            after = []
            for p in range(block):
                four = [v[p] for v in values]
                best = sort_four(*four)
                total = (four[0] + four[1]) + (four[2] + four[3])
                if carry is not None:
                    best = merge_four(carry[p][:TOP], best)
                    total = carry[p][TOP] + total
                after.append(tuple(best) + (total,))
            carry = after
        return carry

    def list_copy(dest):
        return pltpu.make_async_remote_copy(
            src_ref=mine.at[pl.ds(dest * piece, piece)],
            dst_ref=got.at[pl.ds(chip * piece, piece)],
            send_sem=list_send.at[dest],
            recv_sem=list_recv.at[chip],
            device_id={"tmpl": core * targets + dest, "grid": z},
            device_id_type=MESH,
        )

    waited = max(0, groups - 2)
    for g in range(groups):
        if g == waited:
            pl.semaphore_wait(barrier, plane - 1 + 2 * (nz - 1))
            for before in range(g):
                share_stats(before)
        transform(g)
        if g >= waited:
            share_stats(g)
    for g in range(groups):
        pair_copy(g).start()

    for g in range(groups):
        norms(g)
        pair_copy(g).wait_recv()
        if g < groups - 1:

            @pl.loop(0, blocks)
            def _(n):
                where = n * block
                for p, parts in enumerate(best_of(g, where)):
                    for k in range(PARTS):
                        kept[where + p, k] = parts[k]

        else:
            for q in range(nx // 2):
                for low in range(0, rows, block):
                    for p, parts in enumerate(best_of(g, q * rows + low)):
                        for k in range(PARTS):
                            at = q * 8 * piece + k * rows + low + p
                            mine[pl.ds(at, 8, stride=piece), :] = parts[k]
                for k in (2, 1, 3, 0) if ny == 4 else range(ny):
                    for c in range(2):
                        dest = q * 8 + 2 * lax.rem(y + k, ny) + c

                        @pl.when(core * targets + dest != me)
                        def _():
                            list_copy(dest).start()

    source_core = x // (nx // 2)

    @pl.when(source_core == core)
    def _():
        got[pl.ds(chip * piece, piece), :] = mine[pl.ds((me - core * targets) * piece, piece), :]

    @pl.loop(0, targets)
    def _(q):
        @pl.when(2 * q + source_core != me)
        def _():
            pltpu.make_async_remote_copy(
                src_ref=mine.at[pl.ds(0, piece)],
                dst_ref=got.at[pl.ds(q * piece, piece)],
                send_sem=list_send.at[0],
                recv_sem=list_recv.at[q],
                device_id={"tmpl": 2 * q + source_core, "grid": z},
                device_id_type=MESH,
            ).wait_recv()

    lists = []
    total = None
    for q in range(targets):
        parts = [got[q * piece + rows * k : q * piece + rows * (k + 1), :] for k in range(PARTS)]
        lists.append(parts[:TOP])
        total = parts[TOP] if total is None else total + parts[TOP]
    while len(lists) > 1:
        lists = [merge_four(a, b) for a, b in zip(lists[::2], lists[1::2])]
    for k in range(TOP):
        out_ref[k] = lists[0][k]
    out_ref[TOP] = total * (1.0 / math.sqrt(2 * targets * local))

    for g in range(groups):
        pair_copy(g).wait_send()
        for c, peer_z in peers():
            stat_copy(g, own, c, peer_z).wait_send()

    @pl.loop(0, targets)
    def _(dest):
        @pl.when(core * targets + dest != me)
        def _():
            list_copy(dest).wait_send()


def place_kernel(merged, best_ref, sum_ref):
    half = LANES // 2
    for j in range(2):
        part = slice(j * half, (j + 1) * half)
        for k in range(TOP):
            best_ref[k, :, j, :] = merged[k, :, part]
        sum_ref[:, j, :] = merged[TOP, :, part]


def body(sizes, spectrum):
    nx, ny, nz, local = sizes
    points = spectrum.shape[3] // 2
    rows = spectrum.shape[1]
    places = (nx // 2) * rows
    piece = PARTS * rows
    targets = nx * ny
    groups = len(groups_of(local))
    dma = pltpu.SemaphoreType.DMA
    merged = pl.pallas_call(
        functools.partial(kernel, sizes),
        out_shape=jax.ShapeDtypeStruct((PARTS, rows, LANES), jnp.float32),
        in_specs=[pl.BlockSpec(memory_space=pltpu.HBM)],
        out_specs=pl.BlockSpec(memory_space=pltpu.VMEM),
        scratch_shapes=[
            pltpu.VMEM(spectrum.shape, jnp.float32),
            pltpu.VMEM((4 * points, 2 * LANES), jnp.bfloat16),
            pltpu.VMEM((2, local, places, 8, LANES), jnp.float32),
            pltpu.VMEM((local, places, 8, LANES), jnp.float32),
            pltpu.VMEM((local, LANES), jnp.float32),
            pltpu.VMEM((local, LANES), jnp.float32),
            pltpu.VMEM((groups * 2 * nz, 1, LANES), jnp.float32),
            pltpu.VMEM((2, local, LANES), jnp.float32),
            pltpu.VMEM((2, local, LANES), jnp.float32),
            pltpu.VMEM((places, PARTS, 8, LANES), jnp.float32),
            pltpu.VMEM((targets * piece, LANES), jnp.float32),
            pltpu.VMEM((targets * piece, LANES), jnp.float32),
            dma((local // CHUNK,)),
            dma((groups,)),
            dma((groups,)),
            dma((groups * 2 * nz,)),
            dma((groups * 2 * nz,)),
            dma((targets,)),
            dma((targets,)),
        ],
        compiler_params=pltpu.CompilerParams(
            collective_id=0, has_side_effects=True, vmem_limit_bytes=52 * 1024 * 1024
        ),
    )(spectrum)
    return pl.pallas_call(
        place_kernel,
        out_shape=(
            jax.ShapeDtypeStruct((TOP, rows, 2, points), jnp.float32),
            jax.ShapeDtypeStruct((rows, 2, points), jnp.float32),
        ),
        in_specs=[pl.BlockSpec(memory_space=pltpu.VMEM)],
        out_specs=(pl.BlockSpec(memory_space=pltpu.VMEM),) * 2,
        compiler_params=pltpu.CompilerParams(vmem_limit_bytes=1024 * 1024),
    )(merged)


def build(mesh, nx, ny):
    nz = mesh.shape["grid"]

    def run(spectrum):
        sizes = (nx, ny, nz, spectrum.shape[0] // mesh.shape["tmpl"])
        return jax.shard_map(
            functools.partial(body, sizes),
            mesh=mesh,
            in_specs=(P("tmpl", "grid", None, None),),
            out_specs=(P(None, "grid", "tmpl", None), P("grid", "tmpl", None)),
            check_vma=False,
        )(spectrum)

    return run


def solution(mesh):
    return build(mesh, 4, 4)
```

```python
import functools
import math

import jax
import jax.numpy as jnp
from jax import lax
from jax.experimental import pallas as pl
from jax.experimental.pallas import tpu as pltpu
from jax.sharding import PartitionSpec as P

TOP = 4
SPREAD_FLOOR = 0.25
LANES = 128
CHUNK = 2
PARTS = TOP + 1
MESH = pl.DeviceIdType.MESH


def by_distance(size):
    return sorted(range(size), key=lambda k: -min(k, size - k))


def fill_table(table, points):
    shape = (2 * points, LANES)
    row = lax.broadcasted_iota(jnp.int32, shape, 0)
    lane = lax.broadcasted_iota(jnp.int32, shape, 1)
    quarter = jnp.where(row >= points, points // 4, 0)
    turns = ((row & (points - 1)) * (lane & (points - 1)) + quarter) & (points - 1)
    turns = jnp.where(turns > points // 2, turns - points, turns)
    value = jnp.cos(turns.astype(jnp.float32) * (2.0 * math.pi / points))
    high = value.astype(jnp.bfloat16).astype(jnp.float32)
    for parity in range(2):
        keep = (lane >= points) == bool(parity)
        rows = pl.ds(parity * 2 * points, 2 * points)
        table[rows, 0:LANES] = jnp.where(keep, high, 0.0).astype(jnp.bfloat16)
        table[rows, LANES:] = jnp.where(keep, value - high, 0.0).astype(jnp.bfloat16)


def swap(a, b):
    return jnp.maximum(a, b), jnp.minimum(a, b)


def sort_four(a, b, c, d):
    a, b = swap(a, b)
    c, d = swap(c, d)
    a, c = swap(a, c)
    b, d = swap(b, d)
    b, c = swap(b, c)
    return a, b, c, d


def merge_four(first, second):
    a, b, c, d = (jnp.maximum(first[i], second[3 - i]) for i in range(4))
    a, c = swap(a, c)
    b, d = swap(b, d)
    a, b = swap(a, b)
    c, d = swap(c, d)
    return a, b, c, d


def kernel(
    sizes,
    x_hbm,
    out_ref,
    x_buf,
    table,
    score,
    other,
    part_sum,
    part_sq,
    stat,
    scale,
    shift,
    kept,
    mine,
    got,
    x_sem,
    pair_send,
    pair_recv,
    stat_send,
    stat_recv,
    list_send,
    list_recv,
    products,
):
    nx, ny, nz, local = sizes
    chunks = local // CHUNK
    rows = 8
    lines = nx * 8
    piece = PARTS * rows
    targets = nx * ny
    count = float((2 * lines) ** 3)
    cut = local * 3 // 4
    sets = ((0, cut), (cut, local))
    slots = 2 * nz

    me = lax.axis_index("tmpl")
    z = lax.axis_index("grid")
    chip = me // 2
    core = lax.rem(me, 2)
    x = chip // ny
    y = lax.rem(chip, ny)
    sibling = me + 1 - 2 * core
    plane = 2 * targets
    own = core * nz + z

    def load(k):
        return pltpu.make_async_copy(
            x_hbm.at[pl.ds(k * CHUNK, CHUNK)], x_buf.at[pl.ds(k * CHUNK, CHUNK)], x_sem.at[k]
        )

    @pl.loop(0, chunks)
    def _(k):
        load(k).start()

    barrier = pltpu.get_barrier_semaphore()

    for dx in by_distance(nx):
        for dy in by_distance(ny):
            for flip in range(2):
                if dx or dy or flip:
                    c = core if flip == 0 else 1 - core
                    peer = (lax.rem(x + dx, nx) * ny + lax.rem(y + dy, ny)) * 2 + c
                    pl.semaphore_signal(
                        barrier,
                        inc=1,
                        device_id={"tmpl": peer, "grid": z},
                        device_id_type=MESH,
                    )
    for dz in by_distance(nz):
        for c in range(2):
            if dz:
                pl.semaphore_signal(
                    barrier,
                    inc=1,
                    device_id={"tmpl": 2 * chip + c, "grid": lax.rem(z + dz, nz)},
                    device_id_type=MESH,
                )

    fill_table(table, x_hbm.shape[3] // 2)

    def pair_copy(g):
        part = pl.ds(sets[g][0], sets[g][1] - sets[g][0])
        return pltpu.make_async_remote_copy(
            src_ref=score.at[1 - core, part],
            dst_ref=other.at[part],
            send_sem=pair_send.at[g],
            recv_sem=pair_recv.at[g],
            device_id={"tmpl": sibling, "grid": z},
            device_id_type=MESH,
        )

    for unit in range(2):
        for acc in products[unit]:
            pltpu.matmul_pop(acc)
        pltpu.matmul_push_rhs(table[...], staging_register=0, mxu_index=unit)

    def transform(t):
        for part in range(2):
            operands = []
            for parity in range(2):
                value = x_buf[t, :, pl.ds(parity, lines, stride=2), :].reshape(rows * lines, LANES)
                high = value.astype(jnp.bfloat16)
                if part:
                    high = (value - high.astype(jnp.float32)).astype(jnp.bfloat16)
                operands.append(high)
            pltpu.matmul_acc_lhs(
                products[t % 2][t // 2 % 2],
                jnp.concatenate(operands, axis=1),
                load_staged_rhs=0 if t < 2 and part == 0 else None,
            )

    def store(t):
        product = pltpu.matmul_pop(products[t % 2][t // 2 % 2])
        value = (product[:, :LANES] + product[:, LANES:]).reshape(rows, nx, 8, LANES)
        for b in range(nx):
            h, q = b // (nx // 2), b % (nx // 2)
            score[h, t, pl.ds(q * rows, rows)] = value[:, b]
        flat = value.reshape(rows * nx, 8, LANES)
        part_sum[pl.ds(t, 1)] = jnp.sum(jnp.sum(flat, axis=0), axis=0, keepdims=True)
        part_sq[pl.ds(t, 1)] = jnp.sum(jnp.sum(flat * flat, axis=0), axis=0, keepdims=True)

    def masks(n):
        lane = lax.broadcasted_iota(jnp.int32, (n, LANES), 1)
        line = lax.broadcasted_iota(jnp.int32, (n, LANES), 0)
        return lane == line, lane == line + LANES // 2

    def peers():
        for k in by_distance(nz):
            peer_z = lax.rem(z + k, nz)
            for flip in range(2):
                if k or flip:
                    c = core if flip == 0 else 1 - core
                    yield c, peer_z

    def stat_copy(g, slot, c, peer_z):
        return pltpu.make_async_remote_copy(
            src_ref=stat.at[g * slots + slot],
            dst_ref=stat.at[g * slots + slot],
            send_sem=stat_send,
            recv_sem=stat_recv.at[g],
            device_id={"tmpl": 2 * chip + c, "grid": peer_z},
            device_id_type=MESH,
        )

    def share_stats(g):
        low, high = sets[g]
        part = pl.ds(low, high - low)
        first, second = masks(high - low)
        sums = jnp.sum(part_sum[part], axis=1, keepdims=True)
        squares = jnp.sum(part_sq[part], axis=1, keepdims=True)
        line = jnp.where(first, sums, 0.0) + jnp.where(second, squares, 0.0)
        stat[g * slots + own] = jnp.sum(line, axis=0, keepdims=True)
        for c, peer_z in peers():
            stat_copy(g, own, c, peer_z).start()

    def all_stats(g, number):
        both = stat.at[pl.ds(g * slots, number)]
        return pltpu.make_async_remote_copy(
            src_ref=both,
            dst_ref=both,
            send_sem=stat_send,
            recv_sem=stat_recv.at[g],
            device_id={"tmpl": sibling, "grid": z},
            device_id_type=MESH,
        )

    def norms(g):
        all_stats(g, slots - 1).wait_recv()
        low, high = sets[g]
        n = high - low
        part = pl.ds(low, n)
        first, second = masks(n)
        for side in range(2):
            c = core if side == 0 else 1 - core
            line = stat[g * slots + c * nz]
            for k in range(1, nz):
                line = line + stat[g * slots + c * nz + k]
            line = jnp.broadcast_to(line, (n, LANES))
            total = jnp.sum(jnp.where(first, line, 0.0), axis=1, keepdims=True)
            square = jnp.sum(jnp.where(second, line, 0.0), axis=1, keepdims=True)
            average = total / count
            spread = square / count - average * average
            factor = 1.0 / jnp.sqrt(spread + SPREAD_FLOOR)
            scale[side, part] = jnp.broadcast_to(factor, (n, LANES))
            shift[side, part] = jnp.broadcast_to(-average * factor, (n, LANES))

    block = 4
    blocks = (nx // 2) * rows // block

    def best_of(g, where):
        carry = None
        if g:
            carry = [tuple(kept[where + p, k] for k in range(PARTS)) for p in range(block)]
        for t in range(sets[g][0], sets[g][1], 2):
            values = []
            for side in range(2):
                for j in range(2):
                    a = scale[side, pl.ds(t + j, 1), :]
                    b = shift[side, pl.ds(t + j, 1), :]
                    at = pl.ds(where, block)
                    raw = score[core, t + j, at] if side == 0 else other[t + j, at]
                    values.append(raw * a + b)
            after = []
            for p in range(block):
                four = [v[p] for v in values]
                best = sort_four(*four)
                total = (four[0] + four[1]) + (four[2] + four[3])
                if carry is not None:
                    best = merge_four(carry[p][:TOP], best)
                    total = carry[p][TOP] + total
                after.append(tuple(best) + (total,))
            carry = after
        return carry

    def list_copy(dest):
        return pltpu.make_async_remote_copy(
            src_ref=mine.at[pl.ds(dest * piece, piece)],
            dst_ref=got.at[pl.ds(chip * piece, piece)],
            send_sem=list_send,
            recv_sem=list_recv,
            device_id={"tmpl": core * targets + dest, "grid": z},
            device_id_type=MESH,
        )

    for k in range(chunks + 1):
        if k < chunks:
            load(k).wait()
            for t in range(k * CHUNK, (k + 1) * CHUNK):
                transform(t)
        if k:
            for t in range((k - 1) * CHUNK, k * CHUNK):
                store(t)
        if k * CHUNK == cut:
            pl.semaphore_wait(barrier, plane - 1 + 2 * (nz - 1))
            share_stats(0)
    share_stats(1)
    for g in range(2):
        pair_copy(g).start()

    for g in range(2):
        norms(g)
        pair_copy(g).wait_recv()
        if g == 0:

            @pl.loop(0, blocks)
            def _(n):
                where = n * block
                for p, parts in enumerate(best_of(g, where)):
                    for k in range(PARTS):
                        kept[where + p, k] = parts[k]

        else:
            half = nx // 2
            for turn in range(half):
                q = lax.rem((x + 1) // 2 + 1 + core + turn, 2) if half == 2 else turn
                for low in range(0, rows, block):
                    for p, parts in enumerate(best_of(g, q * rows + low)):
                        for k in range(PARTS):
                            at = q * (8 * piece) + (k * rows + low + p)
                            mine[pl.ds(at, 8, stride=piece), :] = parts[k]
                for k in by_distance(ny):
                    for c in range(2):
                        dest = q * 8 + 2 * lax.rem(y + k, ny) + c

                        @pl.when(core * targets + dest != me)
                        def _():
                            list_copy(dest).start()

    source_core = x // (nx // 2)

    @pl.when(source_core == core)
    def _():
        got[pl.ds(chip * piece, piece), :] = mine[pl.ds((me - core * targets) * piece, piece), :]

    all_stats(0, 2 * (slots - 1)).wait_send()
    for g in range(2):
        pair_copy(g).wait_send()

    def all_lists(number):
        return pltpu.make_async_remote_copy(
            src_ref=mine.at[pl.ds(0, number * piece)],
            dst_ref=got.at[pl.ds(0, number * piece)],
            send_sem=list_send,
            recv_sem=list_recv,
            device_id={"tmpl": sibling, "grid": z},
            device_id_type=MESH,
        )

    @pl.when(source_core == core)
    def _():
        all_lists(targets - 1).wait()

    @pl.when(source_core != core)
    def _():
        all_lists(targets).wait()

    lists = []
    total = None
    for q in range(targets):
        parts = [got[q * piece + rows * k : q * piece + rows * (k + 1), :] for k in range(PARTS)]
        lists.append(parts[:TOP])
        total = parts[TOP] if total is None else total + parts[TOP]
    while len(lists) > 1:
        lists = [merge_four(a, b) for a, b in zip(lists[::2], lists[1::2])]
    for k in range(TOP):
        out_ref[k] = lists[0][k]
    out_ref[TOP] = total * (1.0 / math.sqrt(2 * targets * local))


def scoped_kernel(sizes, *refs):
    def run(*products):
        kernel(sizes, *refs, (products[:2], products[2:]))

    rows = 2 * LANES
    pl.run_scoped(run, *(pltpu.ACC(n // 2)((rows, 2 * LANES), jnp.float32) for n in range(4)))


def place_kernel(merged, best_ref, sum_ref):
    half = LANES // 2
    for j in range(2):
        part = slice(j * half, (j + 1) * half)
        for k in range(TOP):
            best_ref[k, :, j, :] = merged[k, :, part]
        sum_ref[:, j, :] = merged[TOP, :, part]


def body(sizes, spectrum):
    nx, ny, nz, local = sizes
    points = spectrum.shape[3] // 2
    rows = spectrum.shape[1]
    places = (nx // 2) * rows
    piece = PARTS * rows
    targets = nx * ny
    dma = pltpu.SemaphoreType.DMA
    merged = pl.pallas_call(
        functools.partial(scoped_kernel, sizes),
        out_shape=jax.ShapeDtypeStruct((PARTS, rows, LANES), jnp.float32),
        in_specs=[pl.BlockSpec(memory_space=pltpu.HBM)],
        out_specs=pl.BlockSpec(memory_space=pltpu.VMEM),
        scratch_shapes=[
            pltpu.VMEM(spectrum.shape, jnp.float32),
            pltpu.VMEM((4 * points, 2 * LANES), jnp.bfloat16),
            pltpu.VMEM((2, local, places, 8, LANES), jnp.float32),
            pltpu.VMEM((local, places, 8, LANES), jnp.float32),
            pltpu.VMEM((local, LANES), jnp.float32),
            pltpu.VMEM((local, LANES), jnp.float32),
            pltpu.VMEM((2 * 2 * nz, 1, LANES), jnp.float32),
            pltpu.VMEM((2, local, LANES), jnp.float32),
            pltpu.VMEM((2, local, LANES), jnp.float32),
            pltpu.VMEM((places, PARTS, 8, LANES), jnp.float32),
            pltpu.VMEM((targets * piece, LANES), jnp.float32),
            pltpu.VMEM((targets * piece, LANES), jnp.float32),
            dma((local // CHUNK,)),
            dma((2,)),
            dma((2,)),
            dma,
            dma((2,)),
            dma,
            dma,
        ],
        compiler_params=pltpu.CompilerParams(
            collective_id=0, has_side_effects=True, vmem_limit_bytes=52 * 1024 * 1024
        ),
    )(spectrum)
    return pl.pallas_call(
        place_kernel,
        out_shape=(
            jax.ShapeDtypeStruct((TOP, rows, 2, points), jnp.float32),
            jax.ShapeDtypeStruct((rows, 2, points), jnp.float32),
        ),
        in_specs=[pl.BlockSpec(memory_space=pltpu.VMEM)],
        out_specs=(pl.BlockSpec(memory_space=pltpu.VMEM),) * 2,
        compiler_params=pltpu.CompilerParams(vmem_limit_bytes=1024 * 1024),
    )(merged)


def build(mesh, nx, ny):
    nz = mesh.shape["grid"]

    def run(spectrum):
        sizes = (nx, ny, nz, spectrum.shape[0] // mesh.shape["tmpl"])
        return jax.shard_map(
            functools.partial(body, sizes),
            mesh=mesh,
            in_specs=(P("tmpl", "grid", None, None),),
            out_specs=(P(None, "grid", "tmpl", None), P("grid", "tmpl", None)),
            check_vma=False,
        )(spectrum)

    return run


def solution(mesh):
    return build(mesh, 4, 4)
```

```python
import functools
import math

import jax
import jax.numpy as jnp
from jax import lax
from jax.experimental import pallas as pl
from jax.experimental.pallas import tpu as pltpu
from jax.sharding import PartitionSpec as P

TOP = 4
SPREAD_FLOOR = 0.25
LANES = 128
CHUNK = 2
PARTS = TOP + 1
MESH = pl.DeviceIdType.MESH


def by_distance(size):
    return sorted(range(size), key=lambda k: -min(k, size - k))


def fill_table(table, points):
    shape = (2 * points, LANES)
    row = lax.broadcasted_iota(jnp.int32, shape, 0)
    lane = lax.broadcasted_iota(jnp.int32, shape, 1)
    quarter = jnp.where(row >= points, points // 4, 0)
    turns = ((row & (points - 1)) * (lane & (points - 1)) + quarter) & (points - 1)
    turns = jnp.where(turns > points // 2, turns - points, turns)
    value = jnp.cos(turns.astype(jnp.float32) * (2.0 * math.pi / points))
    high = value.astype(jnp.bfloat16).astype(jnp.float32)
    for parity in range(2):
        keep = (lane >= points) == bool(parity)
        rows = pl.ds(parity * 2 * points, 2 * points)
        table[rows, 0:LANES] = jnp.where(keep, high, 0.0).astype(jnp.bfloat16)
        table[rows, LANES:] = jnp.where(keep, value - high, 0.0).astype(jnp.bfloat16)


def swap(a, b):
    return jnp.maximum(a, b), jnp.minimum(a, b)


def sort_four(a, b, c, d):
    a, b = swap(a, b)
    c, d = swap(c, d)
    a, c = swap(a, c)
    b, d = swap(b, d)
    b, c = swap(b, c)
    return a, b, c, d


def merge_four(first, second):
    a, b, c, d = (jnp.maximum(first[i], second[3 - i]) for i in range(4))
    a, c = swap(a, c)
    b, d = swap(b, d)
    a, b = swap(a, b)
    c, d = swap(c, d)
    return a, b, c, d


def kernel(
    sizes,
    x_hbm,
    out_ref,
    x_buf,
    table,
    score,
    other,
    part_sum,
    part_sq,
    stat,
    scale,
    shift,
    kept,
    mine,
    got,
    x_sem,
    pair_send,
    pair_recv,
    stat_send,
    stat_recv,
    list_send,
    list_recv,
    products,
):
    nx, ny, nz, local = sizes
    chunks = local // CHUNK
    rows = 8
    lines = nx * 8
    piece = PARTS * rows
    targets = nx * ny
    count = float((2 * lines) ** 3)
    cut = local * 3 // 4
    sets = ((0, cut), (cut, local))
    slots = 2 * nz

    me = lax.axis_index("tmpl")
    z = lax.axis_index("grid")
    chip = me // 2
    core = lax.rem(me, 2)
    x = chip // ny
    y = lax.rem(chip, ny)
    sibling = me + 1 - 2 * core
    plane = 2 * targets
    base = (1 - core) * targets
    own = core * nz + z

    def load(k):
        return pltpu.make_async_copy(
            x_hbm.at[pl.ds(k * CHUNK, CHUNK)], x_buf.at[pl.ds(k * CHUNK, CHUNK)], x_sem.at[k]
        )

    @pl.loop(0, chunks)
    def _(k):
        load(k).start()

    barrier = pltpu.get_barrier_semaphore()

    for dz in by_distance(nz):
        for c in range(2):
            if dz:
                pl.semaphore_signal(
                    barrier,
                    inc=1,
                    device_id={"tmpl": 2 * chip + c, "grid": lax.rem(z + dz, nz)},
                    device_id_type=MESH,
                )
    for dx in by_distance(nx):
        for dy in by_distance(ny):
            for flip in range(2):
                if dx or dy or flip:
                    c = core if flip == 0 else 1 - core
                    peer = (lax.rem(x + dx, nx) * ny + lax.rem(y + dy, ny)) * 2 + c
                    pl.semaphore_signal(
                        barrier,
                        inc=1,
                        device_id={"tmpl": peer, "grid": z},
                        device_id_type=MESH,
                    )

    fill_table(table, x_hbm.shape[3] // 2)

    def pair_copy(g):
        part = pl.ds(sets[g][0], sets[g][1] - sets[g][0])
        return pltpu.make_async_remote_copy(
            src_ref=score.at[core, part],
            dst_ref=other.at[part],
            send_sem=pair_send.at[g],
            recv_sem=pair_recv.at[g],
            device_id={"tmpl": sibling, "grid": z},
            device_id_type=MESH,
        )

    for unit in range(2):
        for acc in products[unit]:
            pltpu.matmul_pop(acc)
        pltpu.matmul_push_rhs(table[...], staging_register=0, mxu_index=unit)

    def transform(t):
        for part in range(2):
            operands = []
            for parity in range(2):
                value = x_buf[t, :, pl.ds(parity, lines, stride=2), :].reshape(rows * lines, LANES)
                high = value.astype(jnp.bfloat16)
                if part:
                    high = (value - high.astype(jnp.float32)).astype(jnp.bfloat16)
                operands.append(high)
            pltpu.matmul_acc_lhs(
                products[t % 2][t // 2 % 2],
                jnp.concatenate(operands, axis=1),
                load_staged_rhs=0 if t < 2 and part == 0 else None,
            )

    def store(t):
        product = pltpu.matmul_pop(products[t % 2][t // 2 % 2])
        value = (product[:, :LANES] + product[:, LANES:]).reshape(rows, nx, 8, LANES)
        for b in range(nx):
            h, q = b // (nx // 2), b % (nx // 2)
            score[h, t, pl.ds(q * rows, rows)] = value[:, b]
        flat = value.reshape(rows * nx, 8, LANES)
        part_sum[pl.ds(t, 1)] = jnp.sum(jnp.sum(flat, axis=0), axis=0, keepdims=True)
        part_sq[pl.ds(t, 1)] = jnp.sum(jnp.sum(flat * flat, axis=0), axis=0, keepdims=True)

    def masks(n):
        lane = lax.broadcasted_iota(jnp.int32, (n, LANES), 1)
        line = lax.broadcasted_iota(jnp.int32, (n, LANES), 0)
        return lane == line, lane == line + LANES // 2

    def peers():
        for k in by_distance(nz):
            peer_z = lax.rem(z + k, nz)
            for flip in range(2):
                if k or flip:
                    c = core if flip == 0 else 1 - core
                    yield c, peer_z

    def stat_copy(g, slot, c, peer_z):
        return pltpu.make_async_remote_copy(
            src_ref=stat.at[g * slots + slot],
            dst_ref=stat.at[g * slots + slot],
            send_sem=stat_send,
            recv_sem=stat_recv.at[g],
            device_id={"tmpl": 2 * chip + c, "grid": peer_z},
            device_id_type=MESH,
        )

    def share_stats(g):
        low, high = sets[g]
        part = pl.ds(low, high - low)
        first, second = masks(high - low)
        sums = jnp.sum(part_sum[part], axis=1, keepdims=True)
        squares = jnp.sum(part_sq[part], axis=1, keepdims=True)
        line = jnp.where(first, sums, 0.0) + jnp.where(second, squares, 0.0)
        stat[g * slots + own] = jnp.sum(line, axis=0, keepdims=True)
        for c, peer_z in peers():
            stat_copy(g, own, c, peer_z).start()

    def all_stats(g, number):
        both = stat.at[pl.ds(g * slots, number)]
        return pltpu.make_async_remote_copy(
            src_ref=both,
            dst_ref=both,
            send_sem=stat_send,
            recv_sem=stat_recv.at[g],
            device_id={"tmpl": sibling, "grid": z},
            device_id_type=MESH,
        )

    def norms(g):
        all_stats(g, slots - 1).wait_recv()
        low, high = sets[g]
        n = high - low
        part = pl.ds(low, n)
        first, second = masks(n)
        for side in range(2):
            c = core if side == 0 else 1 - core
            line = stat[g * slots + c * nz]
            for k in range(1, nz):
                line = line + stat[g * slots + c * nz + k]
            line = jnp.broadcast_to(line, (n, LANES))
            total = jnp.sum(jnp.where(first, line, 0.0), axis=1, keepdims=True)
            square = jnp.sum(jnp.where(second, line, 0.0), axis=1, keepdims=True)
            average = total / count
            spread = square / count - average * average
            factor = 1.0 / jnp.sqrt(spread + SPREAD_FLOOR)
            scale[side, part] = jnp.broadcast_to(factor, (n, LANES))
            shift[side, part] = jnp.broadcast_to(-average * factor, (n, LANES))

    block = 4
    blocks = (nx // 2) * rows // block

    def best_of(g, where):
        carry = None
        if g:
            carry = [tuple(kept[where + p, k] for k in range(PARTS)) for p in range(block)]
        for t in range(sets[g][0], sets[g][1], 2):
            values = []
            for side in range(2):
                for j in range(2):
                    a = scale[side, pl.ds(t + j, 1), :]
                    b = shift[side, pl.ds(t + j, 1), :]
                    at = pl.ds(where, block)
                    raw = score[1 - core, t + j, at] if side == 0 else other[t + j, at]
                    values.append(raw * a + b)
            after = []
            for p in range(block):
                four = [v[p] for v in values]
                best = sort_four(*four)
                total = (four[0] + four[1]) + (four[2] + four[3])
                if carry is not None:
                    best = merge_four(carry[p][:TOP], best)
                    total = carry[p][TOP] + total
                after.append(tuple(best) + (total,))
            carry = after
        return carry

    def list_copy(dest):
        return pltpu.make_async_remote_copy(
            src_ref=mine.at[pl.ds(dest * piece, piece)],
            dst_ref=got.at[pl.ds(chip * piece, piece)],
            send_sem=list_send,
            recv_sem=list_recv,
            device_id={"tmpl": base + dest, "grid": z},
            device_id_type=MESH,
        )

    for k in range(chunks + 1):
        if k < chunks:
            load(k).wait()
            for t in range(k * CHUNK, (k + 1) * CHUNK):
                transform(t)
        if k:
            for t in range((k - 1) * CHUNK, k * CHUNK):
                store(t)
        if k * CHUNK == cut:
            pl.semaphore_wait(barrier, plane - 1 + 2 * (nz - 1))
            share_stats(0)
    share_stats(1)
    for g in range(2):
        pair_copy(g).start()

    for g in range(2):
        norms(g)
        pair_copy(g).wait_recv()
        if g == 0:

            @pl.loop(0, blocks)
            def _(n):
                where = n * block
                for p, parts in enumerate(best_of(g, where)):
                    for k in range(PARTS):
                        kept[where + p, k] = parts[k]

        else:
            half = nx // 2
            for turn in range(half):
                q = turn * core + (1 - core) * lax.rem((x + 1) // 2 + turn, 2) if half == 2 else turn
                for low in range(0, rows, block):
                    for p, parts in enumerate(best_of(g, q * rows + low)):
                        for k in range(PARTS):
                            at = q * (8 * piece) + (k * rows + low + p)
                            mine[pl.ds(at, 8, stride=piece), :] = parts[k]
                if turn == 0:

                    @pl.when((core == 1) & (me != 1))
                    def _():
                        list_copy(1).start()

                for k in by_distance(ny):
                    for c in range(2):
                        dest = q * 8 + 2 * lax.rem(y + k, ny) + c

                        @pl.when((base + dest != me) & (base + dest != 1))
                        def _():
                            list_copy(dest).start()

    source_core = 1 - x // (nx // 2)

    @pl.when(source_core == core)
    def _():
        got[pl.ds(chip * piece, piece), :] = mine[pl.ds((me - base) * piece, piece), :]

    all_stats(0, 2 * (slots - 1)).wait_send()
    for g in range(2):
        pair_copy(g).wait_send()

    def all_lists(number):
        return pltpu.make_async_remote_copy(
            src_ref=mine.at[pl.ds(0, number * piece)],
            dst_ref=got.at[pl.ds(0, number * piece)],
            send_sem=list_send,
            recv_sem=list_recv,
            device_id={"tmpl": sibling, "grid": z},
            device_id_type=MESH,
        )

    @pl.when(source_core == core)
    def _():
        all_lists(targets - 1).wait()

    @pl.when(source_core != core)
    def _():
        all_lists(targets).wait()

    lists = []
    total = None
    for q in range(targets):
        parts = [got[q * piece + rows * k : q * piece + rows * (k + 1), :] for k in range(PARTS)]
        lists.append(parts[:TOP])
        total = parts[TOP] if total is None else total + parts[TOP]
    while len(lists) > 1:
        lists = [merge_four(a, b) for a, b in zip(lists[::2], lists[1::2])]
    for k in range(TOP):
        out_ref[k] = lists[0][k]
    out_ref[TOP] = total * (1.0 / math.sqrt(2 * targets * local))


def scoped_kernel(sizes, *refs):
    def run(*products):
        kernel(sizes, *refs, (products[:2], products[2:]))

    rows = 2 * LANES
    pl.run_scoped(run, *(pltpu.ACC(n // 2)((rows, 2 * LANES), jnp.float32) for n in range(4)))


def place_kernel(merged, best_ref, sum_ref):
    half = LANES // 2
    for j in range(2):
        part = slice(j * half, (j + 1) * half)
        for k in range(TOP):
            best_ref[k, :, j, :] = merged[k, :, part]
        sum_ref[:, j, :] = merged[TOP, :, part]


def body(sizes, spectrum):
    nx, ny, nz, local = sizes
    points = spectrum.shape[3] // 2
    rows = spectrum.shape[1]
    places = (nx // 2) * rows
    piece = PARTS * rows
    targets = nx * ny
    dma = pltpu.SemaphoreType.DMA
    merged = pl.pallas_call(
        functools.partial(scoped_kernel, sizes),
        out_shape=jax.ShapeDtypeStruct((PARTS, rows, LANES), jnp.float32),
        in_specs=[pl.BlockSpec(memory_space=pltpu.HBM)],
        out_specs=pl.BlockSpec(memory_space=pltpu.VMEM),
        scratch_shapes=[
            pltpu.VMEM(spectrum.shape, jnp.float32),
            pltpu.VMEM((4 * points, 2 * LANES), jnp.bfloat16),
            pltpu.VMEM((2, local, places, 8, LANES), jnp.float32),
            pltpu.VMEM((local, places, 8, LANES), jnp.float32),
            pltpu.VMEM((local, LANES), jnp.float32),
            pltpu.VMEM((local, LANES), jnp.float32),
            pltpu.VMEM((2 * 2 * nz, 1, LANES), jnp.float32),
            pltpu.VMEM((2, local, LANES), jnp.float32),
            pltpu.VMEM((2, local, LANES), jnp.float32),
            pltpu.VMEM((places, PARTS, 8, LANES), jnp.float32),
            pltpu.VMEM((targets * piece, LANES), jnp.float32),
            pltpu.VMEM((targets * piece, LANES), jnp.float32),
            dma((local // CHUNK,)),
            dma((2,)),
            dma((2,)),
            dma,
            dma((2,)),
            dma,
            dma,
        ],
        compiler_params=pltpu.CompilerParams(
            collective_id=0, has_side_effects=True, vmem_limit_bytes=52 * 1024 * 1024
        ),
    )(spectrum)
    return pl.pallas_call(
        place_kernel,
        out_shape=(
            jax.ShapeDtypeStruct((TOP, rows, 2, points), jnp.float32),
            jax.ShapeDtypeStruct((rows, 2, points), jnp.float32),
        ),
        in_specs=[pl.BlockSpec(memory_space=pltpu.VMEM)],
        out_specs=(pl.BlockSpec(memory_space=pltpu.VMEM),) * 2,
        compiler_params=pltpu.CompilerParams(vmem_limit_bytes=1024 * 1024),
    )(merged)


def build(mesh, nx, ny):
    nz = mesh.shape["grid"]

    def run(spectrum):
        sizes = (nx, ny, nz, spectrum.shape[0] // mesh.shape["tmpl"])
        return jax.shard_map(
            functools.partial(body, sizes),
            mesh=mesh,
            in_specs=(P("tmpl", "grid", None, None),),
            out_specs=(P(None, "grid", "tmpl", None), P("grid", "tmpl", None)),
            check_vma=False,
        )(spectrum)

    return run


def solution(mesh):
    return build(mesh, 4, 4)
```

```python
import functools
import math

import jax
import jax.numpy as jnp
from jax import lax
from jax.experimental import pallas as pl
from jax.experimental.pallas import tpu as pltpu
from jax.sharding import PartitionSpec as P

TOP = 4
SPREAD_FLOOR = 0.25
LANES = 128
CHUNK = 2
PARTS = TOP + 1
MESH = pl.DeviceIdType.MESH


def by_distance(size):
    return sorted(range(size), key=lambda k: -min(k, size - k))


def fill_table(table, points):
    shape = (2 * points, LANES)
    row = lax.broadcasted_iota(jnp.int32, shape, 0)
    lane = lax.broadcasted_iota(jnp.int32, shape, 1)
    quarter = jnp.where(row >= points, points // 4, 0)
    turns = ((row & (points - 1)) * (lane & (points - 1)) + quarter) & (points - 1)
    turns = jnp.where(turns > points // 2, turns - points, turns)
    value = jnp.cos(turns.astype(jnp.float32) * (2.0 * math.pi / points))
    high = value.astype(jnp.bfloat16).astype(jnp.float32)
    for parity in range(2):
        keep = (lane >= points) == bool(parity)
        rows = pl.ds(parity * 2 * points, 2 * points)
        table[rows, 0:LANES] = jnp.where(keep, high, 0.0).astype(jnp.bfloat16)
        table[rows, LANES:] = jnp.where(keep, value - high, 0.0).astype(jnp.bfloat16)


def swap(a, b):
    return jnp.maximum(a, b), jnp.minimum(a, b)


def sort_four(a, b, c, d):
    a, b = swap(a, b)
    c, d = swap(c, d)
    a, c = swap(a, c)
    b, d = swap(b, d)
    b, c = swap(b, c)
    return a, b, c, d


def merge_four(first, second):
    a, b, c, d = (jnp.maximum(first[i], second[3 - i]) for i in range(4))
    a, c = swap(a, c)
    b, d = swap(b, d)
    a, b = swap(a, b)
    c, d = swap(c, d)
    return a, b, c, d


def kernel(
    sizes,
    x_hbm,
    out_ref,
    x_buf,
    table,
    score,
    other,
    part_sum,
    part_sq,
    stat,
    scale,
    shift,
    kept,
    mine,
    got,
    x_sem,
    pair_send,
    pair_recv,
    stat_send,
    stat_recv,
    list_send,
    list_recv,
    plane_sem,
    products,
):
    nx, ny, nz, local = sizes
    chunks = local // CHUNK
    rows = 8
    lines = nx * 8
    piece = PARTS * rows
    targets = nx * ny
    count = float((2 * lines) ** 3)
    cut = local * 5 // 8 // CHUNK * CHUNK
    sets = ((0, cut), (cut, local))
    slots = 2 * nz

    me = lax.axis_index("tmpl")
    z = lax.axis_index("grid")
    chip = me // 2
    core = lax.rem(me, 2)
    x = chip // ny
    y = lax.rem(chip, ny)
    sibling = me + 1 - 2 * core
    base = (1 - core) * targets
    own = core * nz + z

    def load(k):
        return pltpu.make_async_copy(
            x_hbm.at[pl.ds(k * CHUNK, CHUNK)], x_buf.at[pl.ds(k * CHUNK, CHUNK)], x_sem.at[k]
        )

    @pl.loop(0, chunks)
    def _(k):
        load(k).start()

    barrier = pltpu.get_barrier_semaphore()

    for dz in by_distance(nz):
        for c in range(2):
            if dz:
                pl.semaphore_signal(
                    barrier,
                    inc=1,
                    device_id={"tmpl": 2 * chip + c, "grid": lax.rem(z + dz, nz)},
                    device_id_type=MESH,
                )
    def near():
        for c in range(2):
            for dx in by_distance(nx):
                if dx:
                    yield (lax.rem(x + dx, nx) * ny + y) * 2 + c
            for dy in by_distance(ny):
                if dy:
                    yield (x * ny + lax.rem(y + dy, ny)) * 2 + c
        yield sibling

    def greet(semaphore):
        for peer in near():
            pl.semaphore_signal(
                semaphore, inc=1, device_id={"tmpl": peer, "grid": z}, device_id_type=MESH
            )

    neighbours = 2 * (nx - 1) + 2 * (ny - 1) + 1
    greet(barrier)

    fill_table(table, x_hbm.shape[3] // 2)

    def pair_copy(g):
        part = pl.ds(sets[g][0], sets[g][1] - sets[g][0])
        return pltpu.make_async_remote_copy(
            src_ref=score.at[core, part],
            dst_ref=other.at[part],
            send_sem=pair_send.at[g],
            recv_sem=pair_recv.at[g],
            device_id={"tmpl": sibling, "grid": z},
            device_id_type=MESH,
        )

    for unit in range(2):
        for acc in products[unit]:
            pltpu.matmul_pop(acc)
        pltpu.matmul_push_rhs(table[...], staging_register=0, mxu_index=unit)

    def transform(t):
        for part in range(2):
            operands = []
            for parity in range(2):
                value = x_buf[t, :, pl.ds(parity, lines, stride=2), :].reshape(rows * lines, LANES)
                high = value.astype(jnp.bfloat16)
                if part:
                    high = (value - high.astype(jnp.float32)).astype(jnp.bfloat16)
                operands.append(high)
            pltpu.matmul_acc_lhs(
                products[t % 2][t // 2 % 2],
                jnp.concatenate(operands, axis=1),
                load_staged_rhs=0 if t < 2 and part == 0 else None,
            )

    def store(t):
        product = pltpu.matmul_pop(products[t % 2][t // 2 % 2])
        value = (product[:, :LANES] + product[:, LANES:]).reshape(rows, nx, 8, LANES)
        for b in range(nx):
            h, q = b // (nx // 2), b % (nx // 2)
            score[h, t, pl.ds(q * rows, rows)] = value[:, b]
        flat = value.reshape(rows * nx, 8, LANES)
        part_sum[pl.ds(t, 1)] = jnp.sum(jnp.sum(flat, axis=0), axis=0, keepdims=True)
        part_sq[pl.ds(t, 1)] = jnp.sum(jnp.sum(flat * flat, axis=0), axis=0, keepdims=True)

    def masks(n):
        lane = lax.broadcasted_iota(jnp.int32, (n, LANES), 1)
        line = lax.broadcasted_iota(jnp.int32, (n, LANES), 0)
        return lane == line, lane == line + LANES // 2

    def peers():
        for k in by_distance(nz):
            peer_z = lax.rem(z + k, nz)
            for flip in range(2):
                if k or flip:
                    c = core if flip == 0 else 1 - core
                    yield c, peer_z

    def stat_copy(g, slot, c, peer_z):
        return pltpu.make_async_remote_copy(
            src_ref=stat.at[g * slots + slot],
            dst_ref=stat.at[g * slots + slot],
            send_sem=stat_send,
            recv_sem=stat_recv.at[g],
            device_id={"tmpl": 2 * chip + c, "grid": peer_z},
            device_id_type=MESH,
        )

    def share_stats(g):
        low, high = sets[g]
        part = pl.ds(low, high - low)
        first, second = masks(high - low)
        sums = jnp.sum(part_sum[part], axis=1, keepdims=True)
        squares = jnp.sum(part_sq[part], axis=1, keepdims=True)
        line = jnp.where(first, sums, 0.0) + jnp.where(second, squares, 0.0)
        stat[g * slots + own] = jnp.sum(line, axis=0, keepdims=True)
        for c, peer_z in peers():
            stat_copy(g, own, c, peer_z).start()

    def all_stats(g, number):
        both = stat.at[pl.ds(g * slots, number)]
        return pltpu.make_async_remote_copy(
            src_ref=both,
            dst_ref=both,
            send_sem=stat_send,
            recv_sem=stat_recv.at[g],
            device_id={"tmpl": sibling, "grid": z},
            device_id_type=MESH,
        )

    def norms(g):
        all_stats(g, slots - 1).wait_recv()
        low, high = sets[g]
        n = high - low
        part = pl.ds(low, n)
        first, second = masks(n)
        for side in range(2):
            c = core if side == 0 else 1 - core
            line = stat[g * slots + c * nz]
            for k in range(1, nz):
                line = line + stat[g * slots + c * nz + k]
            line = jnp.broadcast_to(line, (n, LANES))
            total = jnp.sum(jnp.where(first, line, 0.0), axis=1, keepdims=True)
            square = jnp.sum(jnp.where(second, line, 0.0), axis=1, keepdims=True)
            average = total / count
            spread = square / count - average * average
            factor = 1.0 / jnp.sqrt(spread + SPREAD_FLOOR)
            scale[side, part] = jnp.broadcast_to(factor, (n, LANES))
            shift[side, part] = jnp.broadcast_to(-average * factor, (n, LANES))

    block = 4
    blocks = (nx // 2) * rows // block

    def best_of(g, where):
        carry = None
        if g:
            carry = [tuple(kept[where + p, k] for k in range(PARTS)) for p in range(block)]
        for t in range(sets[g][0], sets[g][1], 2):
            values = []
            for side in range(2):
                for j in range(2):
                    a = scale[side, pl.ds(t + j, 1), :]
                    b = shift[side, pl.ds(t + j, 1), :]
                    at = pl.ds(where, block)
                    raw = score[1 - core, t + j, at] if side == 0 else other[t + j, at]
                    values.append(raw * a + b)
            after = []
            for p in range(block):
                four = [v[p] for v in values]
                best = sort_four(*four)
                total = (four[0] + four[1]) + (four[2] + four[3])
                if carry is not None:
                    best = merge_four(carry[p][:TOP], best)
                    total = carry[p][TOP] + total
                after.append(tuple(best) + (total,))
            carry = after
        return carry

    def list_copy(dest):
        return pltpu.make_async_remote_copy(
            src_ref=mine.at[pl.ds(dest * piece, piece)],
            dst_ref=got.at[pl.ds(chip * piece, piece)],
            send_sem=list_send,
            recv_sem=list_recv,
            device_id={"tmpl": base + dest, "grid": z},
            device_id_type=MESH,
        )

    for k in range(chunks + 1):
        if k < chunks:
            load(k).wait()
            for t in range(k * CHUNK, (k + 1) * CHUNK):
                transform(t)
        if k:
            for t in range((k - 1) * CHUNK, k * CHUNK):
                store(t)
        if k * CHUNK == cut:
            pl.semaphore_wait(barrier, neighbours + 2 * (nz - 1))
            share_stats(0)
    share_stats(1)
    for g in range(2):
        pair_copy(g).start()
    greet(plane_sem)

    for g in range(2):
        norms(g)
        pair_copy(g).wait_recv()
        if g == 1:
            pl.semaphore_wait(plane_sem, neighbours)
        if g == 0:

            @pl.loop(0, blocks)
            def _(n):
                where = n * block
                for p, parts in enumerate(best_of(g, where)):
                    for k in range(PARTS):
                        kept[where + p, k] = parts[k]

        else:
            half = nx // 2
            for turn in range(half):
                q = turn * core + (1 - core) * lax.rem((x + 1) // 2 + turn, 2) if half == 2 else turn
                for low in range(0, rows, block):
                    for p, parts in enumerate(best_of(g, q * rows + low)):
                        for k in range(PARTS):
                            at = q * (8 * piece) + (k * rows + low + p)
                            mine[pl.ds(at, 8, stride=piece), :] = parts[k]
                order = [(0, 1)] + [(k, c) for k in by_distance(ny) for c in range(2)]
                for n, (k, c) in enumerate(order):
                    first = q * 8 + 1
                    dest = first if n == 0 else q * 8 + 2 * lax.rem(y + k, ny) + c

                    @pl.when((base + dest != me) & ((dest != first) if n else True))
                    def _():
                        list_copy(dest).start()

    source_core = 1 - x // (nx // 2)

    @pl.when(source_core == core)
    def _():
        got[pl.ds(chip * piece, piece), :] = mine[pl.ds((me - base) * piece, piece), :]

    all_stats(0, 2 * (slots - 1)).wait_send()
    for g in range(2):
        pair_copy(g).wait_send()

    def all_lists(number):
        return pltpu.make_async_remote_copy(
            src_ref=mine.at[pl.ds(0, number * piece)],
            dst_ref=got.at[pl.ds(0, number * piece)],
            send_sem=list_send,
            recv_sem=list_recv,
            device_id={"tmpl": sibling, "grid": z},
            device_id_type=MESH,
        )

    @pl.when(source_core == core)
    def _():
        all_lists(targets - 1).wait()

    @pl.when(source_core != core)
    def _():
        all_lists(targets).wait()

    lists = []
    total = None
    for q in range(targets):
        parts = [got[q * piece + rows * k : q * piece + rows * (k + 1), :] for k in range(PARTS)]
        lists.append(parts[:TOP])
        total = parts[TOP] if total is None else total + parts[TOP]
    while len(lists) > 1:
        lists = [merge_four(a, b) for a, b in zip(lists[::2], lists[1::2])]
    for k in range(TOP):
        out_ref[k] = lists[0][k]
    out_ref[TOP] = total * (1.0 / math.sqrt(2 * targets * local))


def scoped_kernel(sizes, *refs):
    def run(*products):
        kernel(sizes, *refs, (products[:2], products[2:]))

    rows = 2 * LANES
    pl.run_scoped(run, *(pltpu.ACC(n // 2)((rows, 2 * LANES), jnp.float32) for n in range(4)))


def place_kernel(merged, best_ref, sum_ref):
    half = LANES // 2
    for j in range(2):
        part = slice(j * half, (j + 1) * half)
        for k in range(TOP):
            best_ref[k, :, j, :] = merged[k, :, part]
        sum_ref[:, j, :] = merged[TOP, :, part]


def body(sizes, spectrum):
    nx, ny, nz, local = sizes
    points = spectrum.shape[3] // 2
    rows = spectrum.shape[1]
    places = (nx // 2) * rows
    piece = PARTS * rows
    targets = nx * ny
    dma = pltpu.SemaphoreType.DMA
    merged = pl.pallas_call(
        functools.partial(scoped_kernel, sizes),
        out_shape=jax.ShapeDtypeStruct((PARTS, rows, LANES), jnp.float32),
        in_specs=[pl.BlockSpec(memory_space=pltpu.HBM)],
        out_specs=pl.BlockSpec(memory_space=pltpu.VMEM),
        scratch_shapes=[
            pltpu.VMEM(spectrum.shape, jnp.float32),
            pltpu.VMEM((4 * points, 2 * LANES), jnp.bfloat16),
            pltpu.VMEM((2, local, places, 8, LANES), jnp.float32),
            pltpu.VMEM((local, places, 8, LANES), jnp.float32),
            pltpu.VMEM((local, LANES), jnp.float32),
            pltpu.VMEM((local, LANES), jnp.float32),
            pltpu.VMEM((2 * 2 * nz, 1, LANES), jnp.float32),
            pltpu.VMEM((2, local, LANES), jnp.float32),
            pltpu.VMEM((2, local, LANES), jnp.float32),
            pltpu.VMEM((places, PARTS, 8, LANES), jnp.float32),
            pltpu.VMEM((targets * piece, LANES), jnp.float32),
            pltpu.VMEM((targets * piece, LANES), jnp.float32),
            dma((local // CHUNK,)),
            dma((2,)),
            dma((2,)),
            dma,
            dma((2,)),
            dma,
            dma,
            pltpu.SemaphoreType.REGULAR,
        ],
        compiler_params=pltpu.CompilerParams(
            collective_id=0, has_side_effects=True, vmem_limit_bytes=52 * 1024 * 1024
        ),
    )(spectrum)
    return pl.pallas_call(
        place_kernel,
        out_shape=(
            jax.ShapeDtypeStruct((TOP, rows, 2, points), jnp.float32),
            jax.ShapeDtypeStruct((rows, 2, points), jnp.float32),
        ),
        in_specs=[pl.BlockSpec(memory_space=pltpu.VMEM)],
        out_specs=(pl.BlockSpec(memory_space=pltpu.VMEM),) * 2,
        compiler_params=pltpu.CompilerParams(vmem_limit_bytes=1024 * 1024),
    )(merged)


def build(mesh, nx, ny):
    nz = mesh.shape["grid"]

    def run(spectrum):
        sizes = (nx, ny, nz, spectrum.shape[0] // mesh.shape["tmpl"])
        return jax.shard_map(
            functools.partial(body, sizes),
            mesh=mesh,
            in_specs=(P("tmpl", "grid", None, None),),
            out_specs=(P(None, "grid", "tmpl", None), P("grid", "tmpl", None)),
            check_vma=False,
        )(spectrum)

    return run


def solution(mesh):
    return build(mesh, 4, 4)
```

```python
import functools
import math

import jax
import jax.numpy as jnp
from jax import lax
from jax.experimental import pallas as pl
from jax.experimental.pallas import tpu as pltpu
from jax.sharding import PartitionSpec as P

TOP = 4
SPREAD_FLOOR = 0.25
LANES = 128
CHUNK = 2
PARTS = TOP + 1
MESH = pl.DeviceIdType.MESH


def by_distance(size):
    return sorted(range(size), key=lambda k: -min(k, size - k))


def fill_table(table, points):
    shape = (2 * points, LANES)
    row = lax.broadcasted_iota(jnp.int32, shape, 0)
    lane = lax.broadcasted_iota(jnp.int32, shape, 1)
    quarter = jnp.where(row >= points, points // 4, 0)
    turns = ((row & (points - 1)) * (lane & (points - 1)) + quarter) & (points - 1)
    turns = jnp.where(turns > points // 2, turns - points, turns)
    value = jnp.cos(turns.astype(jnp.float32) * (2.0 * math.pi / points))
    high = value.astype(jnp.bfloat16).astype(jnp.float32)
    for parity in range(2):
        keep = (lane >= points) == bool(parity)
        rows = pl.ds(parity * 2 * points, 2 * points)
        table[rows, 0:LANES] = jnp.where(keep, high, 0.0).astype(jnp.bfloat16)
        table[rows, LANES:] = jnp.where(keep, value - high, 0.0).astype(jnp.bfloat16)


def swap(a, b):
    return jnp.maximum(a, b), jnp.minimum(a, b)


def sort_four(a, b, c, d):
    a, b = swap(a, b)
    c, d = swap(c, d)
    a, c = swap(a, c)
    b, d = swap(b, d)
    b, c = swap(b, c)
    return a, b, c, d


def merge_four(first, second):
    a, b, c, d = (jnp.maximum(first[i], second[3 - i]) for i in range(4))
    a, c = swap(a, c)
    b, d = swap(b, d)
    a, b = swap(a, b)
    c, d = swap(c, d)
    return a, b, c, d


def kernel(
    sizes,
    x_hbm,
    out_ref,
    x_buf,
    table,
    score,
    other,
    part_sum,
    part_sq,
    stat,
    scale,
    shift,
    kept,
    mine,
    got,
    x_sem,
    pair_send,
    pair_recv,
    stat_send,
    stat_recv,
    list_send,
    list_recv,
    plane_sem,
    products,
):
    nx, ny, nz, local = sizes
    chunks = local // CHUNK
    rows = 8
    lines = nx * 8
    piece = PARTS * rows
    targets = nx * ny
    count = float((2 * lines) ** 3)
    cut = local * 5 // 8 // CHUNK * CHUNK
    sets = ((0, cut), (cut, local))
    slots = 2 * nz

    me = lax.axis_index("tmpl")
    z = lax.axis_index("grid")
    chip = me // 2
    core = lax.rem(me, 2)
    x = chip // ny
    y = lax.rem(chip, ny)
    sibling = me + 1 - 2 * core

    def step_of(slot):
        return 3 - core + slot * (2 * core - 3)

    def place_of(column):
        step = lax.rem(column - x + nx, nx)
        return lax.rem((step + 1) // 2, 2), 1 - step // 2

    own = core * nz + z

    def load(k):
        return pltpu.make_async_copy(
            x_hbm.at[pl.ds(k * CHUNK, CHUNK)], x_buf.at[pl.ds(k * CHUNK, CHUNK)], x_sem.at[k]
        )

    @pl.loop(0, chunks)
    def _(k):
        load(k).start()

    barrier = pltpu.get_barrier_semaphore()

    for dz in by_distance(nz):
        for c in range(2):
            if dz:
                pl.semaphore_signal(
                    barrier,
                    inc=1,
                    device_id={"tmpl": 2 * chip + c, "grid": lax.rem(z + dz, nz)},
                    device_id_type=MESH,
                )
    def near():
        for c in range(2):
            for dx in by_distance(nx):
                if dx:
                    yield (lax.rem(x + dx, nx) * ny + y) * 2 + c
            for dy in by_distance(ny):
                if dy:
                    yield (x * ny + lax.rem(y + dy, ny)) * 2 + c
        yield sibling

    def greet(semaphore):
        for peer in near():
            pl.semaphore_signal(
                semaphore, inc=1, device_id={"tmpl": peer, "grid": z}, device_id_type=MESH
            )

    neighbours = 2 * (nx - 1) + 2 * (ny - 1) + 1
    greet(barrier)

    fill_table(table, x_hbm.shape[3] // 2)

    def pair_copy(g):
        part = pl.ds(sets[g][0], sets[g][1] - sets[g][0])
        return pltpu.make_async_remote_copy(
            src_ref=score.at[1 - core, part],
            dst_ref=other.at[part],
            send_sem=pair_send.at[g],
            recv_sem=pair_recv.at[g],
            device_id={"tmpl": sibling, "grid": z},
            device_id_type=MESH,
        )

    places_of = [place_of(b) for b in range(nx)]

    for unit in range(2):
        for acc in products[unit]:
            pltpu.matmul_pop(acc)
        pltpu.matmul_push_rhs(table[...], staging_register=0, mxu_index=unit)

    def transform(t):
        for part in range(2):
            operands = []
            for parity in range(2):
                value = x_buf[t, :, pl.ds(parity, lines, stride=2), :].reshape(rows * lines, LANES)
                high = value.astype(jnp.bfloat16)
                if part:
                    high = (value - high.astype(jnp.float32)).astype(jnp.bfloat16)
                operands.append(high)
            pltpu.matmul_acc_lhs(
                products[t % 2][t // 2 % 2],
                jnp.concatenate(operands, axis=1),
                load_staged_rhs=0 if t < 2 and part == 0 else None,
            )

    def store(t):
        product = pltpu.matmul_pop(products[t % 2][t // 2 % 2])
        value = (product[:, :LANES] + product[:, LANES:]).reshape(rows, nx, 8, LANES)
        for b in range(nx):
            h, slot = places_of[b]
            score[h, t, pl.ds(slot * rows, rows)] = value[:, b]
        flat = value.reshape(rows * nx, 8, LANES)
        part_sum[pl.ds(t, 1)] = jnp.sum(jnp.sum(flat, axis=0), axis=0, keepdims=True)
        part_sq[pl.ds(t, 1)] = jnp.sum(jnp.sum(flat * flat, axis=0), axis=0, keepdims=True)

    def masks(n):
        lane = lax.broadcasted_iota(jnp.int32, (n, LANES), 1)
        line = lax.broadcasted_iota(jnp.int32, (n, LANES), 0)
        return lane == line, lane == line + LANES // 2

    def peers():
        for k in by_distance(nz):
            peer_z = lax.rem(z + k, nz)
            for flip in range(2):
                if k or flip:
                    c = core if flip == 0 else 1 - core
                    yield c, peer_z

    def stat_copy(g, slot, c, peer_z):
        return pltpu.make_async_remote_copy(
            src_ref=stat.at[g * slots + slot],
            dst_ref=stat.at[g * slots + slot],
            send_sem=stat_send,
            recv_sem=stat_recv.at[g],
            device_id={"tmpl": 2 * chip + c, "grid": peer_z},
            device_id_type=MESH,
        )

    def share_stats(g):
        low, high = sets[g]
        part = pl.ds(low, high - low)
        first, second = masks(high - low)
        sums = jnp.sum(part_sum[part], axis=1, keepdims=True)
        squares = jnp.sum(part_sq[part], axis=1, keepdims=True)
        line = jnp.where(first, sums, 0.0) + jnp.where(second, squares, 0.0)
        stat[g * slots + own] = jnp.sum(line, axis=0, keepdims=True)
        for c, peer_z in peers():
            stat_copy(g, own, c, peer_z).start()

    def all_stats(g, number):
        both = stat.at[pl.ds(g * slots, number)]
        return pltpu.make_async_remote_copy(
            src_ref=both,
            dst_ref=both,
            send_sem=stat_send,
            recv_sem=stat_recv.at[g],
            device_id={"tmpl": sibling, "grid": z},
            device_id_type=MESH,
        )

    def norms(g):
        all_stats(g, slots - 1).wait_recv()
        low, high = sets[g]
        n = high - low
        part = pl.ds(low, n)
        first, second = masks(n)
        for side in range(2):
            c = core if side == 0 else 1 - core
            line = stat[g * slots + c * nz]
            for k in range(1, nz):
                line = line + stat[g * slots + c * nz + k]
            line = jnp.broadcast_to(line, (n, LANES))
            total = jnp.sum(jnp.where(first, line, 0.0), axis=1, keepdims=True)
            square = jnp.sum(jnp.where(second, line, 0.0), axis=1, keepdims=True)
            average = total / count
            spread = square / count - average * average
            factor = 1.0 / jnp.sqrt(spread + SPREAD_FLOOR)
            scale[side, part] = jnp.broadcast_to(factor, (n, LANES))
            shift[side, part] = jnp.broadcast_to(-average * factor, (n, LANES))

    block = 4
    blocks = (nx // 2) * rows // block

    def best_of(g, where):
        carry = None
        if g:
            carry = [tuple(kept[where + p, k] for k in range(PARTS)) for p in range(block)]
        for t in range(sets[g][0], sets[g][1], 2):
            values = []
            for side in range(2):
                for j in range(2):
                    a = scale[side, pl.ds(t + j, 1), :]
                    b = shift[side, pl.ds(t + j, 1), :]
                    at = pl.ds(where, block)
                    raw = score[core, t + j, at] if side == 0 else other[t + j, at]
                    values.append(raw * a + b)
            after = []
            for p in range(block):
                four = [v[p] for v in values]
                best = sort_four(*four)
                total = (four[0] + four[1]) + (four[2] + four[3])
                if carry is not None:
                    best = merge_four(carry[p][:TOP], best)
                    total = carry[p][TOP] + total
                after.append(tuple(best) + (total,))
            carry = after
        return carry

    def list_copy(slot, line):
        column = lax.rem(x + step_of(slot), nx)
        return pltpu.make_async_remote_copy(
            src_ref=mine.at[pl.ds((slot * 8 + line) * piece, piece)],
            dst_ref=got.at[pl.ds(chip * piece, piece)],
            send_sem=list_send,
            recv_sem=list_recv,
            device_id={"tmpl": column * (2 * ny) + line, "grid": z},
            device_id_type=MESH,
        )

    for k in range(chunks + 1):
        if k < chunks:
            load(k).wait()
            for t in range(k * CHUNK, (k + 1) * CHUNK):
                transform(t)
        if k:
            for t in range((k - 1) * CHUNK, k * CHUNK):
                store(t)
        if k * CHUNK == cut:
            pl.semaphore_wait(barrier, neighbours + 2 * (nz - 1))
            share_stats(0)
    share_stats(1)
    for g in range(2):
        pair_copy(g).start()
    greet(plane_sem)

    for g in range(2):
        norms(g)
        pair_copy(g).wait_recv()
        if g == 1:
            pl.semaphore_wait(plane_sem, neighbours)
        if g == 0:

            @pl.loop(0, blocks)
            def _(n):
                where = n * block
                for p, parts in enumerate(best_of(g, where)):
                    for k in range(PARTS):
                        kept[where + p, k] = parts[k]

        else:
            swap = (1 - core) * (1 - (x + 3) // 4) + core * (x // 3)
            for turn in range(2):
                slot = turn + swap * (1 - 2 * turn)
                for low in range(0, rows, block):
                    for p, parts in enumerate(best_of(g, slot * rows + low)):
                        for k in range(PARTS):
                            at = slot * (8 * piece) + (k * rows + low + p)
                            mine[pl.ds(at, 8, stride=piece), :] = parts[k]
                own_column = (core == 0) & (slot == 1)
                order = [(0, 1)] + [(k, c) for k in by_distance(ny) for c in range(2)]
                for n, (k, c) in enumerate(order):
                    line = 1 if n == 0 else 2 * lax.rem(y + k, ny) + c
                    here = jnp.logical_not(own_column & (line == 2 * y + core))

                    @pl.when(here & ((line != 1) if n else True))
                    def _():
                        list_copy(slot, line).start()

    @pl.when(core == 0)
    def _():
        got[pl.ds(chip * piece, piece), :] = mine[pl.ds((8 + 2 * y) * piece, piece), :]

    all_stats(0, 2 * (slots - 1)).wait_send()
    for g in range(2):
        pair_copy(g).wait_send()

    def all_lists(number):
        return pltpu.make_async_remote_copy(
            src_ref=mine.at[pl.ds(0, number * piece)],
            dst_ref=got.at[pl.ds(0, number * piece)],
            send_sem=list_send,
            recv_sem=list_recv,
            device_id={"tmpl": sibling, "grid": z},
            device_id_type=MESH,
        )

    @pl.when(core == 0)
    def _():
        all_lists(targets - 1).wait()

    @pl.when(core == 1)
    def _():
        all_lists(targets).wait()

    lists = []
    total = None
    for q in range(targets):
        parts = [got[q * piece + rows * k : q * piece + rows * (k + 1), :] for k in range(PARTS)]
        lists.append(parts[:TOP])
        total = parts[TOP] if total is None else total + parts[TOP]
    while len(lists) > 1:
        lists = [merge_four(a, b) for a, b in zip(lists[::2], lists[1::2])]
    for k in range(TOP):
        out_ref[k] = lists[0][k]
    out_ref[TOP] = total * (1.0 / math.sqrt(2 * targets * local))


def scoped_kernel(sizes, *refs):
    def run(*products):
        kernel(sizes, *refs, (products[:2], products[2:]))

    rows = 2 * LANES
    pl.run_scoped(run, *(pltpu.ACC(n // 2)((rows, 2 * LANES), jnp.float32) for n in range(4)))


def place_kernel(merged, best_ref, sum_ref):
    half = LANES // 2
    for j in range(2):
        part = slice(j * half, (j + 1) * half)
        for k in range(TOP):
            best_ref[k, :, j, :] = merged[k, :, part]
        sum_ref[:, j, :] = merged[TOP, :, part]


def body(sizes, spectrum):
    nx, ny, nz, local = sizes
    points = spectrum.shape[3] // 2
    rows = spectrum.shape[1]
    places = (nx // 2) * rows
    piece = PARTS * rows
    targets = nx * ny
    dma = pltpu.SemaphoreType.DMA
    merged = pl.pallas_call(
        functools.partial(scoped_kernel, sizes),
        out_shape=jax.ShapeDtypeStruct((PARTS, rows, LANES), jnp.float32),
        in_specs=[pl.BlockSpec(memory_space=pltpu.HBM)],
        out_specs=pl.BlockSpec(memory_space=pltpu.VMEM),
        scratch_shapes=[
            pltpu.VMEM(spectrum.shape, jnp.float32),
            pltpu.VMEM((4 * points, 2 * LANES), jnp.bfloat16),
            pltpu.VMEM((2, local, places, 8, LANES), jnp.float32),
            pltpu.VMEM((local, places, 8, LANES), jnp.float32),
            pltpu.VMEM((local, LANES), jnp.float32),
            pltpu.VMEM((local, LANES), jnp.float32),
            pltpu.VMEM((2 * 2 * nz, 1, LANES), jnp.float32),
            pltpu.VMEM((2, local, LANES), jnp.float32),
            pltpu.VMEM((2, local, LANES), jnp.float32),
            pltpu.VMEM((places, PARTS, 8, LANES), jnp.float32),
            pltpu.VMEM((targets * piece, LANES), jnp.float32),
            pltpu.VMEM((targets * piece, LANES), jnp.float32),
            dma((local // CHUNK,)),
            dma((2,)),
            dma((2,)),
            dma,
            dma((2,)),
            dma,
            dma,
            pltpu.SemaphoreType.REGULAR,
        ],
        compiler_params=pltpu.CompilerParams(
            collective_id=0, has_side_effects=True, vmem_limit_bytes=52 * 1024 * 1024
        ),
    )(spectrum)
    return pl.pallas_call(
        place_kernel,
        out_shape=(
            jax.ShapeDtypeStruct((TOP, rows, 2, points), jnp.float32),
            jax.ShapeDtypeStruct((rows, 2, points), jnp.float32),
        ),
        in_specs=[pl.BlockSpec(memory_space=pltpu.VMEM)],
        out_specs=(pl.BlockSpec(memory_space=pltpu.VMEM),) * 2,
        compiler_params=pltpu.CompilerParams(vmem_limit_bytes=1024 * 1024),
    )(merged)


def build(mesh, nx, ny):
    nz = mesh.shape["grid"]

    def run(spectrum):
        sizes = (nx, ny, nz, spectrum.shape[0] // mesh.shape["tmpl"])
        return jax.shard_map(
            functools.partial(body, sizes),
            mesh=mesh,
            in_specs=(P("tmpl", "grid", None, None),),
            out_specs=(P(None, "grid", "tmpl", None), P("grid", "tmpl", None)),
            check_vma=False,
        )(spectrum)

    return run


def solution(mesh):
    return build(mesh, 4, 4)
```

```python
import functools
import math

import jax
import jax.numpy as jnp
from jax import lax
from jax.experimental import pallas as pl
from jax.experimental.pallas import tpu as pltpu
from jax.sharding import PartitionSpec as P

TOP = 4
SPREAD_FLOOR = 0.25
LANES = 128
CHUNK = 2
PARTS = TOP + 1
MESH = pl.DeviceIdType.MESH


def by_distance(size):
    return sorted(range(size), key=lambda k: -min(k, size - k))


def fill_table(table, points):
    shape = (2 * points, LANES)
    row = lax.broadcasted_iota(jnp.int32, shape, 0)
    lane = lax.broadcasted_iota(jnp.int32, shape, 1)
    quarter = jnp.where(row >= points, points // 4, 0)
    turns = ((row & (points - 1)) * (lane & (points - 1)) + quarter) & (points - 1)
    turns = jnp.where(turns > points // 2, turns - points, turns)
    value = jnp.cos(turns.astype(jnp.float32) * (2.0 * math.pi / points))
    high = value.astype(jnp.bfloat16).astype(jnp.float32)
    for parity in range(2):
        keep = (lane >= points) == bool(parity)
        rows = pl.ds(parity * 2 * points, 2 * points)
        table[rows, 0:LANES] = jnp.where(keep, high, 0.0).astype(jnp.bfloat16)
        table[rows, LANES:] = jnp.where(keep, value - high, 0.0).astype(jnp.bfloat16)


def swap(a, b):
    return jnp.maximum(a, b), jnp.minimum(a, b)


def sort_four(a, b, c, d):
    a, b = swap(a, b)
    c, d = swap(c, d)
    a, c = swap(a, c)
    b, d = swap(b, d)
    b, c = swap(b, c)
    return a, b, c, d


def merge_four(first, second):
    a, b, c, d = (jnp.maximum(first[i], second[3 - i]) for i in range(4))
    a, c = swap(a, c)
    b, d = swap(b, d)
    a, b = swap(a, b)
    c, d = swap(c, d)
    return a, b, c, d


def kernel(
    sizes,
    x_hbm,
    out_ref,
    x_buf,
    table,
    score,
    other,
    part_sum,
    part_sq,
    stat,
    scale,
    shift,
    kept,
    mine,
    got,
    pair_send,
    pair_recv,
    stat_send,
    stat_recv,
    list_send,
    list_recv,
    plane_sem,
):
    nx, ny, nz, local = sizes
    chunks = local // CHUNK
    rows = 8
    lines = nx * 8
    piece = PARTS * rows
    targets = nx * ny
    count = float((2 * lines) ** 3)
    cut = local * 5 // 8 // CHUNK * CHUNK
    sets = ((0, cut), (cut, local))
    slots = 2 * nz

    me = lax.axis_index("tmpl")
    z = lax.axis_index("grid")
    chip = me // 2
    core = lax.rem(me, 2)
    x = chip // ny
    y = lax.rem(chip, ny)
    sibling = me + 1 - 2 * core

    def step_of(slot):
        return 3 - core + slot * (2 * core - 3)

    def place_of(column):
        step = lax.rem(column - x + nx, nx)
        return lax.rem((step + 1) // 2, 2), 1 - step // 2

    own = core * nz + z

    barrier = pltpu.get_barrier_semaphore()

    def near():
        for c in range(2):
            for dx in by_distance(nx):
                if dx:
                    yield (lax.rem(x + dx, nx) * ny + y) * 2 + c
            for dy in by_distance(ny):
                if dy:
                    yield (x * ny + lax.rem(y + dy, ny)) * 2 + c
        yield sibling

    def greet(semaphore):
        for peer in near():
            pl.semaphore_signal(
                semaphore, inc=1, device_id={"tmpl": peer, "grid": z}, device_id_type=MESH
            )

    neighbours = 2 * (nx - 1) + 2 * (ny - 1) + 1
    def pair_copy(g):
        part = pl.ds(sets[g][0], sets[g][1] - sets[g][0])
        return pltpu.make_async_remote_copy(
            src_ref=score.at[1 - core, part],
            dst_ref=other.at[part],
            send_sem=pair_send,
            recv_sem=pair_recv.at[g],
            device_id={"tmpl": sibling, "grid": z},
            device_id_type=MESH,
        )

    places_of = [place_of(b) for b in range(nx)]

    def masks(n):
        lane = lax.broadcasted_iota(jnp.int32, (n, LANES), 1)
        line = lax.broadcasted_iota(jnp.int32, (n, LANES), 0)
        return lane == line, lane == line + LANES // 2

    def peers():
        for k in by_distance(nz):
            peer_z = lax.rem(z + k, nz)
            for flip in range(2):
                if k or flip:
                    c = core if flip == 0 else 1 - core
                    yield c, peer_z

    def stat_copy(g, slot, c, peer_z):
        return pltpu.make_async_remote_copy(
            src_ref=stat.at[g * slots + slot],
            dst_ref=stat.at[g * slots + slot],
            send_sem=stat_send,
            recv_sem=stat_recv.at[g],
            device_id={"tmpl": 2 * chip + c, "grid": peer_z},
            device_id_type=MESH,
        )

    def share_stats(g):
        low, high = sets[g]
        part = pl.ds(low, high - low)
        first, second = masks(high - low)
        sums = jnp.sum(part_sum[part], axis=1, keepdims=True)
        squares = jnp.sum(part_sq[part], axis=1, keepdims=True)
        line = jnp.where(first, sums, 0.0) + jnp.where(second, squares, 0.0)
        stat[g * slots + own] = jnp.sum(line, axis=0, keepdims=True)
        for c, peer_z in peers():
            stat_copy(g, own, c, peer_z).start()

    def all_stats(g, number):
        both = stat.at[pl.ds(g * slots, number)]
        return pltpu.make_async_remote_copy(
            src_ref=both,
            dst_ref=both,
            send_sem=stat_send,
            recv_sem=stat_recv.at[g],
            device_id={"tmpl": sibling, "grid": z},
            device_id_type=MESH,
        )

    def norms(g):
        all_stats(g, slots - 1).wait_recv()
        low, high = sets[g]
        n = high - low
        part = pl.ds(low, n)
        first, second = masks(n)
        for side in range(2):
            c = core if side == 0 else 1 - core
            line = stat[g * slots + c * nz]
            for k in range(1, nz):
                line = line + stat[g * slots + c * nz + k]
            line = jnp.broadcast_to(line, (n, LANES))
            total = jnp.sum(jnp.where(first, line, 0.0), axis=1, keepdims=True)
            square = jnp.sum(jnp.where(second, line, 0.0), axis=1, keepdims=True)
            average = total / count
            spread = square / count - average * average
            factor = 1.0 / jnp.sqrt(spread + SPREAD_FLOOR)
            scale[side, part] = jnp.broadcast_to(factor, (n, LANES))
            shift[side, part] = jnp.broadcast_to(-average * factor, (n, LANES))

    block = 4
    blocks = (nx // 2) * rows // block

    def best_of(g, where):
        carry = None
        if g:
            carry = [tuple(kept[where + p, k] for k in range(PARTS)) for p in range(block)]
        for t in range(sets[g][0], sets[g][1], 2):
            values = []
            for side in range(2):
                for j in range(2):
                    a = scale[side, pl.ds(t + j, 1), :]
                    b = shift[side, pl.ds(t + j, 1), :]
                    at = pl.ds(where, block)
                    raw = score[core, t + j, at] if side == 0 else other[t + j, at]
                    values.append(raw * a + b)
            after = []
            for p in range(block):
                four = [v[p] for v in values]
                best = sort_four(*four)
                total = (four[0] + four[1]) + (four[2] + four[3])
                if carry is not None:
                    best = merge_four(carry[p][:TOP], best)
                    total = carry[p][TOP] + total
                after.append(tuple(best) + (total,))
            carry = after
        return carry

    def list_copy(slot, line):
        column = lax.rem(x + step_of(slot), nx)
        return pltpu.make_async_remote_copy(
            src_ref=mine.at[pl.ds((slot * 8 + line) * piece, piece)],
            dst_ref=got.at[pl.ds(chip * piece, piece)],
            send_sem=list_send,
            recv_sem=list_recv,
            device_id={"tmpl": column * (2 * ny) + line, "grid": z},
            device_id_type=MESH,
        )

    def transform_all(x_sem, *accumulators):
        products = accumulators[:2], accumulators[2:]

        def load(k):
            return pltpu.make_async_copy(
                x_hbm.at[pl.ds(k * CHUNK, CHUNK)], x_buf.at[pl.ds(k * CHUNK, CHUNK)], x_sem.at[k]
            )

        @pl.loop(0, chunks)
        def _(k):
            load(k).start()

        for dz in by_distance(nz):
            for c in range(2):
                if dz:
                    pl.semaphore_signal(
                        barrier,
                        inc=1,
                        device_id={"tmpl": 2 * chip + c, "grid": lax.rem(z + dz, nz)},
                        device_id_type=MESH,
                    )
        greet(barrier)


        fill_table(table, x_hbm.shape[3] // 2)

        for unit in range(2):
            for acc in products[unit]:
                pltpu.matmul_pop(acc)
            pltpu.matmul_push_rhs(table[...], staging_register=0, mxu_index=unit)

        def transform(t):
            for part in range(2):
                operands = []
                for parity in range(2):
                    value = x_buf[t, :, pl.ds(parity, lines, stride=2), :].reshape(rows * lines, LANES)
                    high = value.astype(jnp.bfloat16)
                    if part:
                        high = (value - high.astype(jnp.float32)).astype(jnp.bfloat16)
                    operands.append(high)
                pltpu.matmul_acc_lhs(
                    products[t % 2][t // 2 % 2],
                    jnp.concatenate(operands, axis=1),
                    load_staged_rhs=0 if t < 2 and part == 0 else None,
                )

        def store(t):
            product = pltpu.matmul_pop(products[t % 2][t // 2 % 2])
            value = (product[:, :LANES] + product[:, LANES:]).reshape(rows, nx, 8, LANES)
            for b in range(nx):
                h, slot = places_of[b]
                score[h, t, pl.ds(slot * rows, rows)] = value[:, b]
            flat = value.reshape(rows * nx, 8, LANES)
            part_sum[pl.ds(t, 1)] = jnp.sum(jnp.sum(flat, axis=0), axis=0, keepdims=True)
            part_sq[pl.ds(t, 1)] = jnp.sum(jnp.sum(flat * flat, axis=0), axis=0, keepdims=True)

        for k in range(chunks + 1):
            if k < chunks:
                load(k).wait()
                for t in range(k * CHUNK, (k + 1) * CHUNK):
                    transform(t)
            if k:
                for t in range((k - 1) * CHUNK, k * CHUNK):
                    store(t)
            if k * CHUNK == cut:
                pl.semaphore_wait(barrier, neighbours + 2 * (nz - 1))
                share_stats(0)
        share_stats(1)
        for g in range(2):
            pair_copy(g).start()
        greet(plane_sem)

    wide = 2 * LANES
    pl.run_scoped(
        transform_all,
        pltpu.SemaphoreType.DMA((chunks,)),
        *(pltpu.ACC(n // 2)((wide, wide), jnp.float32) for n in range(4)),
    )

    for g in range(2):
        norms(g)
        pair_copy(g).wait_recv()
        if g == 1:
            pl.semaphore_wait(plane_sem, neighbours)
        if g == 0:

            @pl.loop(0, blocks)
            def _(n):
                where = n * block
                for p, parts in enumerate(best_of(g, where)):
                    for k in range(PARTS):
                        kept[where + p, k] = parts[k]

        else:
            swap = (1 - core) * (1 - (x + 3) // 4) + core * (x // 3)
            for turn in range(2):
                slot = turn + swap * (1 - 2 * turn)
                for low in range(0, rows, block):
                    for p, parts in enumerate(best_of(g, slot * rows + low)):
                        for k in range(PARTS):
                            at = slot * (8 * piece) + (k * rows + low + p)
                            mine[pl.ds(at, 8, stride=piece), :] = parts[k]
                own_column = (core == 0) & (slot == 1)
                order = [(0, 1)] + [(k, c) for k in by_distance(ny) for c in range(2)]
                for n, (k, c) in enumerate(order):
                    line = 1 if n == 0 else 2 * lax.rem(y + k, ny) + c
                    here = jnp.logical_not(own_column & (line == 2 * y + core))

                    @pl.when(here & ((line != 1) if n else True))
                    def _():
                        list_copy(slot, line).start()

    @pl.when(core == 0)
    def _():
        got[pl.ds(chip * piece, piece), :] = mine[pl.ds((8 + 2 * y) * piece, piece), :]

    all_stats(0, 2 * (slots - 1)).wait_send()
    pltpu.make_async_remote_copy(
        src_ref=score.at[1 - core],
        dst_ref=other,
        send_sem=pair_send,
        recv_sem=pair_recv.at[0],
        device_id={"tmpl": sibling, "grid": z},
        device_id_type=MESH,
    ).wait_send()

    def all_lists(number):
        return pltpu.make_async_remote_copy(
            src_ref=mine.at[pl.ds(0, number * piece)],
            dst_ref=got.at[pl.ds(0, number * piece)],
            send_sem=list_send,
            recv_sem=list_recv,
            device_id={"tmpl": sibling, "grid": z},
            device_id_type=MESH,
        )

    @pl.when(core == 0)
    def _():
        all_lists(targets - 1).wait()

    @pl.when(core == 1)
    def _():
        all_lists(targets).wait()

    lists = []
    total = None
    for q in range(targets):
        parts = [got[q * piece + rows * k : q * piece + rows * (k + 1), :] for k in range(PARTS)]
        lists.append(parts[:TOP])
        total = parts[TOP] if total is None else total + parts[TOP]
    while len(lists) > 1:
        lists = [merge_four(a, b) for a, b in zip(lists[::2], lists[1::2])]
    for k in range(TOP):
        out_ref[k] = lists[0][k]
    out_ref[TOP] = total * (1.0 / math.sqrt(2 * targets * local))


def place_kernel(merged, best_ref, sum_ref):
    half = LANES // 2
    for j in range(2):
        part = slice(j * half, (j + 1) * half)
        for k in range(TOP):
            best_ref[k, :, j, :] = merged[k, :, part]
        sum_ref[:, j, :] = merged[TOP, :, part]


def body(sizes, spectrum):
    nx, ny, nz, local = sizes
    points = spectrum.shape[3] // 2
    rows = spectrum.shape[1]
    places = (nx // 2) * rows
    piece = PARTS * rows
    targets = nx * ny
    dma = pltpu.SemaphoreType.DMA
    merged = pl.pallas_call(
        functools.partial(kernel, sizes),
        out_shape=jax.ShapeDtypeStruct((PARTS, rows, LANES), jnp.float32),
        in_specs=[pl.BlockSpec(memory_space=pltpu.HBM)],
        out_specs=pl.BlockSpec(memory_space=pltpu.VMEM),
        scratch_shapes=[
            pltpu.VMEM(spectrum.shape, jnp.float32),
            pltpu.VMEM((4 * points, 2 * LANES), jnp.bfloat16),
            pltpu.VMEM((2, local, places, 8, LANES), jnp.float32),
            pltpu.VMEM((local, places, 8, LANES), jnp.float32),
            pltpu.VMEM((local, LANES), jnp.float32),
            pltpu.VMEM((local, LANES), jnp.float32),
            pltpu.VMEM((2 * 2 * nz, 1, LANES), jnp.float32),
            pltpu.VMEM((2, local, LANES), jnp.float32),
            pltpu.VMEM((2, local, LANES), jnp.float32),
            pltpu.VMEM((places, PARTS, 8, LANES), jnp.float32),
            pltpu.VMEM((targets * piece, LANES), jnp.float32),
            pltpu.VMEM((targets * piece, LANES), jnp.float32),
            dma,
            dma((2,)),
            dma,
            dma((2,)),
            dma,
            dma,
            pltpu.SemaphoreType.REGULAR,
        ],
        compiler_params=pltpu.CompilerParams(
            collective_id=0, has_side_effects=True, vmem_limit_bytes=52 * 1024 * 1024
        ),
    )(spectrum)
    return pl.pallas_call(
        place_kernel,
        out_shape=(
            jax.ShapeDtypeStruct((TOP, rows, 2, points), jnp.float32),
            jax.ShapeDtypeStruct((rows, 2, points), jnp.float32),
        ),
        in_specs=[pl.BlockSpec(memory_space=pltpu.VMEM)],
        out_specs=(pl.BlockSpec(memory_space=pltpu.VMEM),) * 2,
        compiler_params=pltpu.CompilerParams(vmem_limit_bytes=1024 * 1024),
    )(merged)


def build(mesh, nx, ny):
    nz = mesh.shape["grid"]

    def run(spectrum):
        sizes = (nx, ny, nz, spectrum.shape[0] // mesh.shape["tmpl"])
        return jax.shard_map(
            functools.partial(body, sizes),
            mesh=mesh,
            in_specs=(P("tmpl", "grid", None, None),),
            out_specs=(P(None, "grid", "tmpl", None), P("grid", "tmpl", None)),
            check_vma=False,
        )(spectrum)

    return run


def solution(mesh):
    return build(mesh, 4, 4)
```

```python
import functools
import math

import jax
import jax.numpy as jnp
from jax import lax
from jax.experimental import pallas as pl
from jax.experimental.pallas import tpu as pltpu
from jax.sharding import PartitionSpec as P

TOP = 4
SPREAD_FLOOR = 0.25
LANES = 128
CHUNK = 2
PARTS = TOP + 1
MESH = pl.DeviceIdType.MESH


def by_distance(size):
    return sorted(range(size), key=lambda k: -min(k, size - k))


def fill_table(table, points):
    shape = (2 * points, LANES)
    row = lax.broadcasted_iota(jnp.int32, shape, 0)
    lane = lax.broadcasted_iota(jnp.int32, shape, 1)
    quarter = jnp.where(row >= points, points // 4, 0)
    turns = ((row & (points - 1)) * (lane & (points - 1)) + quarter) & (points - 1)
    turns = jnp.where(turns > points // 2, turns - points, turns)
    value = jnp.cos(turns.astype(jnp.float32) * (2.0 * math.pi / points))
    high = value.astype(jnp.bfloat16).astype(jnp.float32)
    for parity in range(2):
        keep = (lane >= points) == bool(parity)
        rows = pl.ds(parity * 2 * points, 2 * points)
        table[rows, 0:LANES] = jnp.where(keep, high, 0.0).astype(jnp.bfloat16)
        table[rows, LANES:] = jnp.where(keep, value - high, 0.0).astype(jnp.bfloat16)


def swap(a, b):
    return jnp.maximum(a, b), jnp.minimum(a, b)


def sort_four(a, b, c, d):
    a, b = swap(a, b)
    c, d = swap(c, d)
    a, c = swap(a, c)
    b, d = swap(b, d)
    b, c = swap(b, c)
    return a, b, c, d


def merge_four(first, second):
    a, b, c, d = (jnp.maximum(first[i], second[3 - i]) for i in range(4))
    a, c = swap(a, c)
    b, d = swap(b, d)
    a, b = swap(a, b)
    c, d = swap(c, d)
    return a, b, c, d


def kernel(
    sizes,
    x_hbm,
    out_ref,
    x_buf,
    table,
    score,
    other,
    part_sum,
    part_sq,
    stat,
    scale,
    shift,
    kept,
    mine,
    got,
    pair_send,
    pair_recv,
    stat_send,
    stat_recv,
    list_send,
    list_recv,
    plane_sem,
):
    nx, ny, nz, local = sizes
    chunks = local // CHUNK
    rows = 8
    lines = nx * 8
    piece = PARTS * rows
    targets = nx * ny
    count = float((2 * lines) ** 3)
    cut = local * 5 // 8 // CHUNK * CHUNK
    sets = ((0, cut), (cut, local))
    slots = 2 * nz

    me = lax.axis_index("tmpl")
    z = lax.axis_index("grid")
    chip = me // 2
    core = lax.rem(me, 2)
    x = chip // ny
    y = lax.rem(chip, ny)
    sibling = me + 1 - 2 * core

    def step_of(slot):
        return 3 - core + slot * (2 * core - 3)

    def place_of(column):
        step = lax.rem(column - x + nx, nx)
        return lax.rem((step + 1) // 2, 2), 1 - step // 2

    own = core * nz + z

    barrier = pltpu.get_barrier_semaphore()

    def near():
        for c in range(2):
            for dx in by_distance(nx):
                if dx:
                    yield (lax.rem(x + dx, nx) * ny + y) * 2 + c
            for dy in by_distance(ny):
                if dy:
                    yield (x * ny + lax.rem(y + dy, ny)) * 2 + c
        yield sibling

    def greet(semaphore):
        for peer in near():
            pl.semaphore_signal(
                semaphore, inc=1, device_id={"tmpl": peer, "grid": z}, device_id_type=MESH
            )

    neighbours = 2 * (nx - 1) + 2 * (ny - 1) + 1
    def pair_copy(g):
        part = pl.ds(sets[g][0], sets[g][1] - sets[g][0])
        return pltpu.make_async_remote_copy(
            src_ref=score.at[1 - core, part],
            dst_ref=other.at[part],
            send_sem=pair_send,
            recv_sem=pair_recv.at[g],
            device_id={"tmpl": sibling, "grid": z},
            device_id_type=MESH,
        )

    places_of = [place_of(b) for b in range(nx)]

    def masks(n):
        lane = lax.broadcasted_iota(jnp.int32, (n, LANES), 1)
        line = lax.broadcasted_iota(jnp.int32, (n, LANES), 0)
        return lane == line, lane == line + LANES // 2

    def peers():
        for k in by_distance(nz):
            peer_z = lax.rem(z + k, nz)
            for flip in range(2):
                if k or flip:
                    c = core if flip == 0 else 1 - core
                    yield c, peer_z

    def stat_copy(g, slot, c, peer_z):
        return pltpu.make_async_remote_copy(
            src_ref=stat.at[g * slots + slot],
            dst_ref=stat.at[g * slots + slot],
            send_sem=stat_send,
            recv_sem=stat_recv.at[g],
            device_id={"tmpl": 2 * chip + c, "grid": peer_z},
            device_id_type=MESH,
        )

    def share_stats(g):
        low, high = sets[g]
        part = pl.ds(low, high - low)
        first, second = masks(high - low)
        sums = jnp.sum(part_sum[part], axis=1, keepdims=True)
        squares = jnp.sum(part_sq[part], axis=1, keepdims=True)
        line = jnp.where(first, sums, 0.0) + jnp.where(second, squares, 0.0)
        stat[g * slots + own] = jnp.sum(line, axis=0, keepdims=True)
        for c, peer_z in peers():
            stat_copy(g, own, c, peer_z).start()

    def all_stats(g, number):
        both = stat.at[pl.ds(g * slots, number)]
        return pltpu.make_async_remote_copy(
            src_ref=both,
            dst_ref=both,
            send_sem=stat_send,
            recv_sem=stat_recv.at[g],
            device_id={"tmpl": sibling, "grid": z},
            device_id_type=MESH,
        )

    def norms(g):
        all_stats(g, slots - 1).wait_recv()
        low, high = sets[g]
        n = high - low
        part = pl.ds(low, n)
        first, second = masks(n)
        for side in range(2):
            c = core if side == 0 else 1 - core
            line = stat[g * slots + c * nz]
            for k in range(1, nz):
                line = line + stat[g * slots + c * nz + k]
            line = jnp.broadcast_to(line, (n, LANES))
            total = jnp.sum(jnp.where(first, line, 0.0), axis=1, keepdims=True)
            square = jnp.sum(jnp.where(second, line, 0.0), axis=1, keepdims=True)
            average = total / count
            spread = square / count - average * average
            factor = 1.0 / jnp.sqrt(spread + SPREAD_FLOOR)
            scale[side, part] = jnp.broadcast_to(factor, (n, LANES))
            shift[side, part] = jnp.broadcast_to(-average * factor, (n, LANES))

    block = 4
    blocks = (nx // 2) * rows // block

    def best_of(g, where):
        carry = None
        if g:
            carry = [tuple(kept[where + p, k] for k in range(PARTS)) for p in range(block)]
        for t in range(sets[g][0], sets[g][1], 2):
            values = []
            for side in range(2):
                for j in range(2):
                    a = scale[side, pl.ds(t + j, 1), :]
                    b = shift[side, pl.ds(t + j, 1), :]
                    at = pl.ds(where, block)
                    raw = score[core, t + j, at] if side == 0 else other[t + j, at]
                    values.append(raw * a + b)
            after = []
            for p in range(block):
                four = [v[p] for v in values]
                best = sort_four(*four)
                total = (four[0] + four[1]) + (four[2] + four[3])
                if carry is not None:
                    best = merge_four(carry[p][:TOP], best)
                    total = carry[p][TOP] + total
                after.append(tuple(best) + (total,))
            carry = after
        return carry

    def list_copy(slot, line):
        column = lax.rem(x + step_of(slot), nx)
        return pltpu.make_async_remote_copy(
            src_ref=mine.at[pl.ds((slot * 8 + line) * piece, piece)],
            dst_ref=got.at[pl.ds(chip * piece, piece)],
            send_sem=list_send,
            recv_sem=list_recv,
            device_id={"tmpl": column * (2 * ny) + line, "grid": z},
            device_id_type=MESH,
        )

    def transform_all(x_sem, *accumulators):
        products = accumulators[:2], accumulators[2:]

        def load(k):
            return pltpu.make_async_copy(
                x_hbm.at[pl.ds(k * CHUNK, CHUNK)], x_buf.at[pl.ds(k * CHUNK, CHUNK)], x_sem.at[k]
            )

        @pl.loop(0, chunks)
        def _(k):
            load(k).start()

        for dz in by_distance(nz):
            for c in range(2):
                if dz:
                    pl.semaphore_signal(
                        barrier,
                        inc=1,
                        device_id={"tmpl": 2 * chip + c, "grid": lax.rem(z + dz, nz)},
                        device_id_type=MESH,
                    )
        greet(barrier)


        fill_table(table, x_hbm.shape[3] // 2)

        for unit in range(2):
            for acc in products[unit]:
                pltpu.matmul_pop(acc)
            pltpu.matmul_push_rhs(table[...], staging_register=0, mxu_index=unit)

        def transform(t):
            for part in range(2):
                operands = []
                for parity in range(2):
                    value = x_buf[t, :, pl.ds(parity, lines, stride=2), :].reshape(rows * lines, LANES)
                    high = value.astype(jnp.bfloat16)
                    if part:
                        high = (value - high.astype(jnp.float32)).astype(jnp.bfloat16)
                    operands.append(high)
                pltpu.matmul_acc_lhs(
                    products[t % 2][t // 2 % 2],
                    jnp.concatenate(operands, axis=1),
                    load_staged_rhs=0 if t < 2 and part == 0 else None,
                )

        def store(t):
            product = pltpu.matmul_pop(products[t % 2][t // 2 % 2])
            value = (product[:, :LANES] + product[:, LANES:]).reshape(rows, nx, 8, LANES)
            for b in range(nx):
                h, slot = places_of[b]
                score[h, t, pl.ds(slot * rows, rows)] = value[:, b]
            flat = value.reshape(rows * nx, 8, LANES)
            part_sum[pl.ds(t, 1)] = jnp.sum(jnp.sum(flat, axis=0), axis=0, keepdims=True)
            part_sq[pl.ds(t, 1)] = jnp.sum(jnp.sum(flat * flat, axis=0), axis=0, keepdims=True)

        for k in range(chunks + 1):
            if k < chunks:
                load(k).wait()
                for t in range(k * CHUNK, (k + 1) * CHUNK):
                    transform(t)
            if k:
                for t in range((k - 1) * CHUNK, k * CHUNK):
                    store(t)
            if k * CHUNK == cut:
                pl.semaphore_wait(barrier, neighbours + 2 * (nz - 1))
                share_stats(0)
        share_stats(1)
        for g in range(2):
            pair_copy(g).start()
        greet(plane_sem)

    wide = 2 * LANES
    pl.run_scoped(
        transform_all,
        pltpu.SemaphoreType.DMA((chunks,)),
        *(pltpu.ACC(n // 2)((wide, wide), jnp.float32) for n in range(4)),
    )

    for g in range(2):
        norms(g)
        pair_copy(g).wait_recv()
        if g == 1:
            pl.semaphore_wait(plane_sem, neighbours)
        if g == 0:

            @pl.loop(0, blocks)
            def _(n):
                where = n * block
                for p, parts in enumerate(best_of(g, where)):
                    for k in range(PARTS):
                        kept[where + p, k] = parts[k]

        else:
            swap = (1 - core) * (1 - (x + 3) // 4) + core * (x // 3)
            for turn in range(2):
                slot = turn + swap * (1 - 2 * turn)
                for low in range(0, rows, block):
                    for p, parts in enumerate(best_of(g, slot * rows + low)):
                        for k in range(PARTS):
                            at = slot * (8 * piece) + (k * rows + low + p)
                            mine[pl.ds(at, 8, stride=piece), :] = parts[k]
                own_column = (core == 0) & (slot == 1)
                order = [(0, 1)] * (turn == 0) + [(k, c) for k in by_distance(ny) for c in (1, 0)]
                for n, (k, c) in enumerate(order):
                    line = 1 if n + turn == 0 else 2 * lax.rem(y + k, ny) + c
                    here = jnp.logical_not(own_column & (line == 2 * y + core))

                    @pl.when(here & ((line != 1) if n and turn == 0 else True))
                    def _():
                        list_copy(slot, line).start()

    @pl.when(core == 0)
    def _():
        got[pl.ds(chip * piece, piece), :] = mine[pl.ds((8 + 2 * y) * piece, piece), :]

    all_stats(0, 2 * (slots - 1)).wait_send()
    pltpu.make_async_remote_copy(
        src_ref=score.at[1 - core],
        dst_ref=other,
        send_sem=pair_send,
        recv_sem=pair_recv.at[0],
        device_id={"tmpl": sibling, "grid": z},
        device_id_type=MESH,
    ).wait_send()

    def all_lists(number):
        return pltpu.make_async_remote_copy(
            src_ref=mine.at[pl.ds(0, number * piece)],
            dst_ref=got.at[pl.ds(0, number * piece)],
            send_sem=list_send,
            recv_sem=list_recv,
            device_id={"tmpl": sibling, "grid": z},
            device_id_type=MESH,
        )

    @pl.when(core == 0)
    def _():
        all_lists(targets - 1).wait()

    @pl.when(core == 1)
    def _():
        all_lists(targets).wait()

    lists = []
    total = None
    for q in range(targets):
        parts = [got[q * piece + rows * k : q * piece + rows * (k + 1), :] for k in range(PARTS)]
        lists.append(parts[:TOP])
        total = parts[TOP] if total is None else total + parts[TOP]
    while len(lists) > 1:
        lists = [merge_four(a, b) for a, b in zip(lists[::2], lists[1::2])]
    for k in range(TOP):
        out_ref[k] = lists[0][k]
    out_ref[TOP] = total * (1.0 / math.sqrt(2 * targets * local))


def place_kernel(merged, best_ref, sum_ref):
    half = LANES // 2
    for j in range(2):
        part = slice(j * half, (j + 1) * half)
        for k in range(TOP):
            best_ref[k, :, j, :] = merged[k, :, part]
        sum_ref[:, j, :] = merged[TOP, :, part]


def body(sizes, spectrum):
    nx, ny, nz, local = sizes
    points = spectrum.shape[3] // 2
    rows = spectrum.shape[1]
    places = (nx // 2) * rows
    piece = PARTS * rows
    targets = nx * ny
    dma = pltpu.SemaphoreType.DMA
    merged = pl.pallas_call(
        functools.partial(kernel, sizes),
        out_shape=jax.ShapeDtypeStruct((PARTS, rows, LANES), jnp.float32),
        in_specs=[pl.BlockSpec(memory_space=pltpu.HBM)],
        out_specs=pl.BlockSpec(memory_space=pltpu.VMEM),
        scratch_shapes=[
            pltpu.VMEM(spectrum.shape, jnp.float32),
            pltpu.VMEM((4 * points, 2 * LANES), jnp.bfloat16),
            pltpu.VMEM((2, local, places, 8, LANES), jnp.float32),
            pltpu.VMEM((local, places, 8, LANES), jnp.float32),
            pltpu.VMEM((local, LANES), jnp.float32),
            pltpu.VMEM((local, LANES), jnp.float32),
            pltpu.VMEM((2 * 2 * nz, 1, LANES), jnp.float32),
            pltpu.VMEM((2, local, LANES), jnp.float32),
            pltpu.VMEM((2, local, LANES), jnp.float32),
            pltpu.VMEM((places, PARTS, 8, LANES), jnp.float32),
            pltpu.VMEM((targets * piece, LANES), jnp.float32),
            pltpu.VMEM((targets * piece, LANES), jnp.float32),
            dma,
            dma((2,)),
            dma,
            dma((2,)),
            dma,
            dma,
            pltpu.SemaphoreType.REGULAR,
        ],
        compiler_params=pltpu.CompilerParams(
            collective_id=0, has_side_effects=True, vmem_limit_bytes=52 * 1024 * 1024
        ),
    )(spectrum)
    return pl.pallas_call(
        place_kernel,
        out_shape=(
            jax.ShapeDtypeStruct((TOP, rows, 2, points), jnp.float32),
            jax.ShapeDtypeStruct((rows, 2, points), jnp.float32),
        ),
        in_specs=[pl.BlockSpec(memory_space=pltpu.VMEM)],
        out_specs=(pl.BlockSpec(memory_space=pltpu.VMEM),) * 2,
        compiler_params=pltpu.CompilerParams(vmem_limit_bytes=1024 * 1024),
    )(merged)


def build(mesh, nx, ny):
    nz = mesh.shape["grid"]

    def run(spectrum):
        sizes = (nx, ny, nz, spectrum.shape[0] // mesh.shape["tmpl"])
        return jax.shard_map(
            functools.partial(body, sizes),
            mesh=mesh,
            in_specs=(P("tmpl", "grid", None, None),),
            out_specs=(P(None, "grid", "tmpl", None), P("grid", "tmpl", None)),
            check_vma=False,
        )(spectrum)

    return run


def solution(mesh):
    return build(mesh, 4, 4)
```
